256 devices in a mesh: lon: 4 (over y), lat: 4 (over x), mem: 16 (over z, core).
Axes of the slice: x: 4, y: 4, z: 8, core: 2. Of those that a mesh axis runs over, the one named last changes fastest.
Arguments:
- north_vel: bfloat16 [16, 4, 75, 128, 512], P('mem', None, None, 'lat', 'lon'), may hold values from -6 to 6
- up_vel: bfloat16 [16, 4, 75, 128, 512], P('mem', None, None, 'lat', 'lon'), may hold values from -6 to 6
- dens_class: int32 [16, 4, 75, 128, 512], P('mem', None, None, 'lat', 'lon'), may hold values from 0 to 79
- thickness: int32 [75, 128, 512], P(None, 'lat', 'lon'), may hold values from 0 to 2000
- basin_id: int32 [128, 512], P('lat', 'lon'), may hold values from 0 to 3
Outputs:
- depth_mean: float32 [4, 4, 2, 75, 128], P('lon', None, None, None, 'lat')
- depth_spread: float32 [4, 4, 2, 75, 128], P('lon', None, None, None, 'lat')
- class_mean: float32 [4, 4, 2, 80, 128], P('lon', None, None, None, 'lat')
- class_spread: float32 [4, 4, 2, 80, 128], P('lon', None, None, None, 'lat')
The draws below stay inside these ranges and needn't reach their ends.
Inputs may be any that keep to these rules, and one draw needn't show every extreme that they name: `basin_id`: 0 marks land; 1 to 3 name the basins. `thickness`: thousandths of a unit layer; 0 marks a cell below the sea floor.
All inputs are finite; a program needn't handle non-finite values.
Results may differ from the reference program's by a relative error of at most 0.0029.
Values sent between devices are 32-bit elements; how exact they have to be, the bound alone decides.
A program may use at most 128 MiB of HBM per device.

```python
import math
import jax
import jax.numpy as jnp
from jax import lax

MONTHS = 4
LEVELS = 75
CLASSES = 80
BASINS = 3
NLON = 512
NLAT = 128
MEMBERS = 16


def place_ends(array, rng, least, top_value):
    extent = array.shape
    index_at = [jax.random.randint(jax.random.fold_in(rng, axis), (), 0, extent[axis]) for axis in range(len(extent))]
    array = array.at[tuple(index_at)].set(least)
    longest = extent.index(max(extent))
    index_at[longest] = (index_at[longest] + 1) % extent[longest]
    return array.at[tuple(index_at)].set(top_value)


def level_of(own_key, extent, shards, low, top_value):
    factor_of, own = 1.0, jax.random.fold_in(own_key, 6)
    for position, shards_of in shards:
        heights = jnp.exp(jax.random.uniform(jax.random.fold_in(own, position), (shards_of,), jnp.float32, low / len(shards), top_value / len(shards)))
        factor_of = factor_of * jnp.repeat(heights, extent[position] // shards_of).reshape([-1 if axis == position else 1 for axis in range(len(extent))])
    return factor_of


def scatter_about(own_key, shape, width, most, pieces=(), held_as=jnp.bfloat16):
    entries = width * jax.random.normal(own_key, shape, jnp.float32)
    if pieces:
        entries = entries * level_of(own_key, shape, pieces, -0.22, 0.18)
    return jnp.clip(entries, -most, most).astype(held_as)


def setup_inputs(seed: int = 0) -> dict:
    arg_keys = jax.random.split(jax.random.key(seed), 6)
    north_vel = scatter_about(arg_keys[0], (MEMBERS, MONTHS, LEVELS, NLAT, NLON), 1.0, 6.0, ((0, 16), (3, 4), (4, 4)))
    up_vel = scatter_about(arg_keys[1], (MEMBERS, MONTHS, LEVELS, NLAT, NLON), 1.0, 6.0, ((0, 16), (3, 4), (4, 4)))
    dens_class = place_ends(jax.random.randint(arg_keys[2], (MEMBERS, MONTHS, LEVELS, NLAT, NLON), 0, CLASSES), jax.random.fold_in(arg_keys[2], 1), 0, CLASSES - 1).astype(jnp.int32)
    thickness = place_ends(jax.random.randint(arg_keys[3], (LEVELS, NLAT, NLON), 0, 2001), jax.random.fold_in(arg_keys[3], 1), 0, 2000).astype(jnp.int32)
    basin_id = place_ends(jax.random.randint(arg_keys[4], (NLAT, NLON), 0, BASINS + 1), jax.random.fold_in(arg_keys[4], 1), 0, BASINS).astype(jnp.int32)
    return {"north_vel": north_vel, "up_vel": up_vel, "dens_class": dens_class, "thickness": thickness, "basin_id": basin_id}


north_unit = 0.02
up_unit = 0.01

def class_sums(north_flux, rise_flux, dens_class, basin_masks):
    months, levels, lat_rows, lon_cells = north_flux.shape
    weighted = jnp.stack([north_flux, rise_flux], 2).reshape(months * levels, 2, lat_rows, lon_cells)
    classes_flat = dens_class.reshape(months * levels, lat_rows, lon_cells)
    class_ids = jnp.arange(CLASSES, dtype=jnp.int32)

    def one_level(packed):
        onehot = (packed[1][..., None] == class_ids).astype(jnp.float32)
        return jnp.einsum('sji,bji,jic->bscj', packed[0], basin_masks, onehot, precision=lax.Precision.HIGHEST)
    per_level = lax.map(one_level, (weighted, classes_flat))
    return lax.optimization_barrier(jnp.sum(per_level.reshape(months, levels, BASINS, 2, CLASSES, lat_rows), axis=1))

def member_tables(north_vel, up_vel, dens_class, thickness, basin_id, first_row, lat_total):
    months, levels, lat_rows, lon_cells = north_vel.shape
    row_index = first_row + jnp.arange(lat_rows, dtype=jnp.int32)
    latitude = (-78.0 + 156.0 * (row_index.astype(jnp.float32) + 0.5) / lat_total) * (math.pi / 180.0)
    zonal_width = jnp.cos(latitude)
    layer_depth = thickness.astype(jnp.float32) * 0.001
    wet_cells = (thickness > 0).astype(jnp.float32)
    north_flux = north_vel.astype(jnp.float32) * (north_unit * zonal_width)[None, None, :, None] * layer_depth[None]
    rise_flux = up_vel.astype(jnp.float32) * (up_unit * zonal_width)[None, None, :, None] * wet_cells[None]
    north_flux = north_flux.astype(jnp.bfloat16).astype(jnp.float32)
    rise_flux = rise_flux.astype(jnp.bfloat16).astype(jnp.float32)
    basin_masks = (basin_id[None] == jnp.arange(1, BASINS + 1, dtype=jnp.int32)[:, None, None]).astype(jnp.float32)
    north_depth = jnp.einsum('mkji,bji->mbkj', north_flux, basin_masks, precision=lax.Precision.HIGHEST)
    rise_depth = jnp.einsum('mkji,bji->mbkj', rise_flux, basin_masks, precision=lax.Precision.HIGHEST)
    depth_tab = jnp.stack([north_depth, rise_depth], 2)
    class_tab = class_sums(north_flux, rise_flux, dens_class, basin_masks)
    return (class_tab, depth_tab)

def with_global(tables):
    return jnp.concatenate([lax.optimization_barrier(jnp.sum(tables, axis=2, keepdims=True)), tables], 2)

def moments(stack_moc):
    members = stack_moc.shape[0]
    mean_val = lax.optimization_barrier(jnp.sum(stack_moc, 0)) / members
    spread_val = jnp.sqrt(lax.optimization_barrier(jnp.sum(jnp.square(stack_moc - mean_val), 0)) / (members - 1))
    return (mean_val, spread_val)

def reference(north_vel, up_vel, dens_class, thickness, basin_id):

    def one_member(packed):
        return member_tables(packed[0], packed[1], packed[2], thickness, basin_id, 0, NLAT)
    class_tab, depth_tab = lax.map(one_member, (north_vel, up_vel, dens_class))
    class_reg = with_global(class_tab)
    depth_reg = with_global(depth_tab)
    class_moc = jnp.stack([jnp.cumsum(class_reg[:, :, :, 0], axis=3), jnp.cumsum(jnp.cumsum(class_reg[:, :, :, 1], axis=4), axis=3)], 3)
    depth_moc = jnp.stack([jnp.cumsum(depth_reg[:, :, :, 0], axis=3), jnp.cumsum(depth_reg[:, :, :, 1], axis=4)], 3)
    depth_mean, depth_spread = moments(depth_moc)
    class_mean, class_spread = moments(class_moc)
    return (depth_mean, depth_spread, class_mean, class_spread)
```

```python
import functools
import math

import jax
import jax.numpy as jnp
from jax import lax
from jax.experimental import pallas as pl
from jax.experimental.pallas import tpu as pltpu
from jax.sharding import PartitionSpec as P

CLASSES = 80
BASINS = 3


north_unit = 0.02
up_unit = 0.01


def cut_along(shard, dim, devices):
    dims = shard.shape
    parts = shard.reshape(*dims[:dim], devices, dims[dim] // devices, *dims[dim + 1 :])
    return jnp.moveaxis(parts, dim, 0)


def summed_on_arrival(shard, axis, dim):
    devices = lax.axis_size(axis)
    parts = lax.all_to_all(cut_along(shard, dim, devices), axis, 0, 0, tiled=True)
    return jnp.sum(parts, axis=0)


def in_one_piece(arrays, axis, dim, along):
    ends, at = ([], 0)
    for a in arrays[:-1]:
        at += a.shape[along]
        ends.append(at)
    both = jnp.concatenate(arrays, axis=along)
    return tuple(jnp.split(summed_on_arrival(both, axis, dim), ends, axis=along))


def in_one_piece_2(arrays, axis, dim, along):
    ends, at = ([], 0)
    for a in arrays[:-1]:
        at += a.shape[along]
        ends.append(at)
    both = jnp.concatenate(arrays, axis=along)
    return tuple(jnp.split(lax.all_gather(both, axis, axis=dim, tiled=True), ends, axis=along))


def filled_up(lines, devices):
    spare = -lines.shape[0] % devices
    if not spare:
        return lines
    return jnp.concatenate([lines, jnp.zeros((spare, *lines.shape[1:]), lines.dtype)])


def sent_to_all(shard, axis):
    copies = jnp.broadcast_to(shard, (lax.axis_size(axis), *shard.shape))
    return lax.all_to_all(copies, axis, split_axis=0, concat_axis=0, tiled=True)


def in_order(parts, dim):
    parts = jnp.moveaxis(parts, 0, dim)
    dims = parts.shape
    return parts.reshape(*dims[:dim], dims[dim] * dims[dim + 1], *dims[dim + 2 :])


def gather_directly(shard, axis, dim):
    parts = sent_to_all(shard, axis)
    return in_order(parts, dim)


def nested_sum(shard, axes):
    padded = filled_up(shard, lax.axis_size(axes))
    whole = gather_directly(summed_on_arrival(padded, axes, 0), axes, 0)
    return lax.slice_in_dim(whole, 0, len(shard)).reshape(shard.shape)


def packed_total(arrays, axis):
    ends = [0]
    for a in arrays:
        ends.append(ends[-1] + a.size)
    subtotal = nested_sum(jnp.concatenate([a.ravel() for a in arrays]), axis)
    return tuple((subtotal[b:e].reshape(a.shape) for a, b, e in zip(arrays, ends, ends[1:])))


NT = (((1,), (1,)), ((), ()))

def tables_kernel(lat_axis, pairs, rounds, n_ref, u_ref, c_ref, th_ref, b_ref, t_ref, d_ref,
                  cn_ref, cr_ref, hb_ref, mk_ref, acc_ref, f_ref):
    levels, rows, lons = th_ref.shape
    groups = rows // 8
    bf = jnp.bfloat16
    f32 = jnp.float32

    @pl.when(pl.program_id(0) == 0)
    def _():
        first = (lax.axis_index(lat_axis) if lat_axis else 0) * rows
        j = lax.broadcasted_iota(jnp.int32, (rows, lons), 0) + first
        phi = (-78.0 + 156.0 * (j.astype(f32) + 0.5) / 128) * (math.pi / 180.0)
        zw = jnp.cos(phi)

        @pl.loop(0, levels)
        def _(k):
            th = th_ref[k]
            cn_ref[k] = (0.02 * zw) * (th.astype(f32) * 0.001)
            cr_ref[k] = jnp.where(th > 0, 0.01 * zw, 0.0)

        for k in range(levels, cn_ref.shape[0]):
            cn_ref[k] = jnp.zeros((rows, lons), f32)
            cr_ref[k] = jnp.zeros((rows, lons), f32)
        b = b_ref[...]
        hb_ref[...] = jnp.where(b > 0, (b - 1) * 5, -100)
        z = jnp.zeros((128, lons), bf)
        m = jnp.concatenate([(b == v).astype(f32) for v in (1, 2, 3)] + [jnp.zeros((rows, lons), f32)], 0).astype(bf)
        mk_ref[...] = jnp.concatenate(
            [jnp.concatenate([m, z], 1), jnp.concatenate([z, m], 1)], 0)

    zero = jnp.zeros((16, lons), bf)
    one = jnp.ones((16, lons), bf)

    def build(k, tile):
        kk = jnp.minimum(k, levels - 1)
        r0 = 16 * tile
        nf = n_ref[0, kk, r0:r0 + 16, :].astype(f32) * cn_ref[k, r0:r0 + 16, :]
        rf = u_ref[0, kk, r0:r0 + 16, :].astype(f32) * cr_ref[k, r0:r0 + 16, :]
        cc = c_ref[0, kk, r0:r0 + 16, :]
        hi = ((cc >> 4) + hb_ref[r0:r0 + 16, :]).astype(f32)
        lo = (cc & 15).astype(f32)
        out = []
        for s in range(2):
            a, b = nf[8 * s:8 * s + 8], rf[8 * s:8 * s + 8]
            h, l = hi[8 * s:8 * s + 8], lo[8 * s:8 * s + 8]
            nn = jnp.concatenate([a, a], 0).astype(bf)
            rr = jnp.concatenate([b, b], 0).astype(bf)
            fl = jnp.concatenate([a, b], 0).astype(bf)
            hh = jnp.concatenate([h, h - 1.0], 0).astype(bf)
            ll = jnp.concatenate([l, l - 1.0], 0).astype(bf)
            S = [jnp.where(hh == bf(2 * q), one, zero) for q in range(8)]
            ms = [ll == bf(2 * q) for q in range(8)]
            P = [jnp.where(m, nn, zero) for m in ms] + [jnp.where(m, rr, zero) for m in ms]
            out.append((jnp.concatenate(S, 0), jnp.concatenate(P, 0), fl))
        return out

    def chunk(base, first):
        for tile in range(groups // 2):
            got = [[], []]
            for t in range(2 * pairs):
                for s, item in enumerate(build(base + t, tile)):
                    got[s].append(item)
            for s in range(2):
                g = 2 * tile + s
                S = jnp.concatenate([x[0] for x in got[s]], 1)
                P = jnp.concatenate([x[1] for x in got[s]], 1)
                r = lax.dot_general(S, P, NT, preferred_element_type=f32)
                acc_ref[g] = r if first else acc_ref[g] + r
                for p in range(pairs):
                    f_ref[base // 2 + p, 16 * g:16 * g + 16, :] = jnp.concatenate(
                        [got[s][2 * p][2], got[s][2 * p + 1][2]], 1)

    for g in range(groups):
        acc_ref[g] = jnp.zeros(acc_ref.shape[1:], f32)

    @pl.loop(0, rounds)
    def _(r):
        chunk(r * 2 * pairs, False)

    i_row = lax.broadcasted_iota(jnp.int32, (8, 256), 0)
    i_col = lax.broadcasted_iota(jnp.int32, (8, 256), 1)
    keep = (i_col % 8) == i_row
    for g in range(groups):
        x = acc_ref[g].reshape(16, 8, 256)
        t_ref[0, g] = jnp.sum(jnp.where(keep[None], x, 0.0), axis=1)

    npairs = pairs * rounds
    d_row = lax.broadcasted_iota(jnp.int32, (8, 256), 0)
    d_col = lax.broadcasted_iota(jnp.int32, (8, 256), 1)

    nb = f_ref.shape[0]
    F = f_ref[...].reshape(nb * 16 * groups, 256)
    R = lax.dot_general(F, mk_ref[...], NT, preferred_element_type=f32).reshape(nb, groups, 2, 8, 256)
    tot = 0.0
    for g in range(groups):
        tot = tot + jnp.where((d_col % 32) == d_row + 8 * g, R[:, g], 0.0)
    tot = jnp.sum(tot, axis=2)
    d_ref[0] = tot


def tables(north, up, dens, thick, basin, lat_axis=None, pairs=19, rounds=2):
    months, levels, rows, lons = north.shape
    groups = rows // 8
    npairs = pairs * rounds
    big = lambda: pl.BlockSpec((1, levels, rows, lons), lambda m: (m, 0, 0, 0))
    return pl.pallas_call(
        functools.partial(tables_kernel, lat_axis, pairs, rounds),
        grid=(months,),
        in_specs=[big(), big(), big(),
                  pl.BlockSpec((levels, rows, lons), lambda m: (0, 0, 0), pipeline_mode=pl.Buffered(1)),
                  pl.BlockSpec((rows, lons), lambda m: (0, 0), pipeline_mode=pl.Buffered(1))],
        out_specs=[pl.BlockSpec((1, groups, 16, 256), lambda m: (m, 0, 0, 0)),
                   pl.BlockSpec((1, npairs, 2, 256), lambda m: (m, 0, 0, 0))],
        out_shape=[jax.ShapeDtypeStruct((months, groups, 16, 256), jnp.float32),
                   jax.ShapeDtypeStruct((months, npairs, 2, 256), jnp.float32)],
        scratch_shapes=[
            pltpu.VMEM((2 * npairs, rows, lons), jnp.float32),
            pltpu.VMEM((2 * npairs, rows, lons), jnp.float32),
            pltpu.VMEM((rows, lons), jnp.int32),
            pltpu.VMEM((256, 256), jnp.bfloat16),
            pltpu.VMEM((groups, 128, 256), jnp.float32),
            pltpu.VMEM((npairs, 16 * groups, 256), jnp.bfloat16),
        ],
        compiler_params=pltpu.CompilerParams(vmem_limit_bytes=60 * 2**20),
        name="tables",
    )(north, up, dens, thick, basin)

def whole_tables(north_vel, up_vel, dens_class, thickness, basin_id):
    t, d = tables(north_vel[0], up_vel[0], dens_class[0], thickness, basin_id, "lat")
    months, groups = t.shape[:2]
    t = t.reshape(months, groups, 16, 2, 16, 8)[:, :, :15]
    class_tab = t.reshape(months, groups, 3, 5, 2, 16, 8).transpose(0, 2, 4, 3, 5, 1, 6)
    class_tab = class_tab.reshape(1, months, 3, 2, 80, groups * 8)
    levels = thickness.shape[0]
    d = d.reshape(months, -1, 2, 2, 4, groups * 8).transpose(0, 4, 2, 1, 3, 5)
    depth_tab = d.reshape(months, 4, 2, -1, groups * 8)[None, :, :3, :, :levels]
    return class_tab, depth_tab


def with_global(tables):
    return jnp.concatenate([jnp.sum(tables, axis=2, keepdims=True), tables], 2)


def body(north_vel, up_vel, dens_class, thickness, basin_id):
    class_tab, depth_tab = whole_tables(north_vel, up_vel, dens_class, thickness, basin_id)
    class_tab, depth_tab = in_one_piece((class_tab, depth_tab), "lon", 1, 4)
    class_reg = with_global(class_tab)
    depth_reg = with_global(depth_tab)
    class_block = jnp.sum(class_reg[:, :, :, 1], axis=-1)
    depth_block = jnp.sum(depth_reg[:, :, :, 1], axis=-1)
    all_class, all_depth = in_one_piece_2((class_block[None], depth_block[None]), "lat", 0, 4)
    below_mask = (jnp.arange(all_class.shape[0], dtype=jnp.int32) < lax.axis_index("lat")).astype(
        jnp.float32
    )
    carry_class = jnp.sum(all_class * below_mask[:, None, None, None, None], axis=0)
    carry_depth = jnp.sum(all_depth * below_mask[:, None, None, None, None], axis=0)
    class_south = jnp.cumsum(class_reg[:, :, :, 1], axis=4) + carry_class[..., None]
    class_moc = jnp.stack(
        [jnp.cumsum(class_reg[:, :, :, 0], axis=3), jnp.cumsum(class_south, axis=3)], 3
    )
    depth_south = jnp.cumsum(depth_reg[:, :, :, 1], axis=4) + carry_depth[..., None]
    depth_moc = jnp.stack([jnp.cumsum(depth_reg[:, :, :, 0], axis=3), depth_south], 3)
    members = class_moc.shape[0] * lax.axis_size("mem")
    class_total, depth_total, class_square, depth_square = packed_total(
        (
            jnp.sum(class_moc, 0),
            jnp.sum(depth_moc, 0),
            jnp.sum(jnp.square(class_moc), 0),
            jnp.sum(jnp.square(depth_moc), 0),
        ),
        "mem",
    )
    class_mean = class_total / members
    depth_mean = depth_total / members
    class_spread = jnp.sqrt(
        jnp.maximum((class_square - class_total * class_mean) / (members - 1), 0.0)
    )
    depth_spread = jnp.sqrt(
        jnp.maximum((depth_square - depth_total * depth_mean) / (members - 1), 0.0)
    )
    return (depth_mean, depth_spread, class_mean, class_spread)


def solution(mesh):
    in_specs = (
        P("mem", None, None, "lat", "lon"),
        P("mem", None, None, "lat", "lon"),
        P("mem", None, None, "lat", "lon"),
        P(None, "lat", "lon"),
        P("lat", "lon"),
    )
    out_specs = (
        P("lon", None, None, None, "lat"),
        P("lon", None, None, None, "lat"),
        P("lon", None, None, None, "lat"),
        P("lon", None, None, None, "lat"),
    )
    return jax.shard_map(body, mesh=mesh, in_specs=in_specs, out_specs=out_specs, check_vma=False)
```

```python
import functools
import math

import jax
import jax.numpy as jnp
from jax import lax
from jax.experimental import pallas as pl
from jax.experimental.pallas import tpu as pltpu
from jax.sharding import PartitionSpec as P

NT = (((1,), (1,)), ((), ()))

def tables_kernel(lat_axis, lat_total, pairs, rounds, n_ref, u_ref, c_ref, th_ref, b_ref, t_ref, d_ref,
                  cn_ref, cr_ref, hb_ref, mk_ref, acc_ref, f_ref):
    levels, rows, lons = th_ref.shape
    groups = rows // 8
    bf = jnp.bfloat16
    f32 = jnp.float32

    @pl.when(pl.program_id(0) == 0)
    def _():
        first = (lax.axis_index(lat_axis) if lat_axis else 0) * rows
        j = lax.broadcasted_iota(jnp.int32, (rows, lons), 0) + first
        phi = (-78.0 + 156.0 * (j.astype(f32) + 0.5) / lat_total) * (math.pi / 180.0)
        zw = jnp.cos(phi)

        @pl.loop(0, levels)
        def _(k):
            th = th_ref[k]
            cn_ref[k] = (0.02 * zw) * (th.astype(f32) * 0.001)
            cr_ref[k] = jnp.where(th > 0, 0.01 * zw, 0.0)

        for k in range(levels, cn_ref.shape[0]):
            cn_ref[k] = jnp.zeros((rows, lons), f32)
            cr_ref[k] = jnp.zeros((rows, lons), f32)
        b = b_ref[...]
        hb_ref[...] = jnp.where(b > 0, (b - 1) * 5, -100)
        z = jnp.zeros((128, lons), bf)
        m = jnp.concatenate([(b == v).astype(f32) for v in (1, 2, 3)] + [jnp.zeros((128 - 3 * rows, lons), f32)], 0).astype(bf)
        mk_ref[...] = jnp.concatenate(
            [jnp.concatenate([m, z], 1), jnp.concatenate([z, m], 1)], 0)

    zero = jnp.zeros((16, lons), bf)
    one = jnp.ones((16, lons), bf)

    def build(k, tile):
        kk = jnp.minimum(k, levels - 1)
        r0 = 16 * tile
        nf = n_ref[0, kk, r0:r0 + 16, :].astype(f32) * cn_ref[k, r0:r0 + 16, :]
        rf = u_ref[0, kk, r0:r0 + 16, :].astype(f32) * cr_ref[k, r0:r0 + 16, :]
        cc = c_ref[0, kk, r0:r0 + 16, :]
        hi = ((cc >> 4) + hb_ref[r0:r0 + 16, :]).astype(f32)
        lo = (cc & 15).astype(f32)
        out = []
        for s in range(2):
            a, b = nf[8 * s:8 * s + 8], rf[8 * s:8 * s + 8]
            h, l = hi[8 * s:8 * s + 8], lo[8 * s:8 * s + 8]
            nn = jnp.concatenate([a, a], 0).astype(bf)
            rr = jnp.concatenate([b, b], 0).astype(bf)
            fl = jnp.concatenate([a, b], 0).astype(bf)
            hh = jnp.concatenate([h, h - 1.0], 0).astype(bf)
            ll = jnp.concatenate([l, l - 1.0], 0).astype(bf)
            S = [jnp.where(hh == bf(2 * q), one, zero) for q in range(8)]
            ms = [ll == bf(2 * q) for q in range(8)]
            P = [jnp.where(m, nn, zero) for m in ms] + [jnp.where(m, rr, zero) for m in ms]
            out.append((jnp.concatenate(S, 0), jnp.concatenate(P, 0), fl))
        return out

    def chunk(base, first):
        for tile in range(groups // 2):
            got = [[], []]
            for t in range(2 * pairs):
                for s, item in enumerate(build(base + t, tile)):
                    got[s].append(item)
            for s in range(2):
                g = 2 * tile + s
                S = jnp.concatenate([x[0] for x in got[s]], 1)
                P = jnp.concatenate([x[1] for x in got[s]], 1)
                r = lax.dot_general(S, P, NT, preferred_element_type=f32)
                acc_ref[g] = r if first else acc_ref[g] + r
                for p in range(pairs):
                    f_ref[base // 2 + p, 16 * g:16 * g + 16, :] = jnp.concatenate(
                        [got[s][2 * p][2], got[s][2 * p + 1][2]], 1)

    for g in range(groups):
        acc_ref[g] = jnp.zeros(acc_ref.shape[1:], f32)

    @pl.loop(0, rounds)
    def _(r):
        chunk(r * 2 * pairs, False)

    i_row = lax.broadcasted_iota(jnp.int32, (8, 256), 0)
    i_col = lax.broadcasted_iota(jnp.int32, (8, 256), 1)
    keep = (i_col % 8) == i_row
    for g in range(groups):
        x = acc_ref[g].reshape(16, 8, 256)
        t_ref[0, g] = jnp.sum(jnp.where(keep[None], x, 0.0), axis=1)

    npairs = pairs * rounds
    d_row = lax.broadcasted_iota(jnp.int32, (8, 256), 0)
    d_col = lax.broadcasted_iota(jnp.int32, (8, 256), 1)

    nb = f_ref.shape[0]
    F = f_ref[...].reshape(nb * 16 * groups, 256)
    R = lax.dot_general(F, mk_ref[...], NT, preferred_element_type=f32).reshape(nb, groups, 2, 8, 256)
    for f in range(2):
        tot = 0.0
        for g in range(groups):
            tot = tot + jnp.where((d_col % rows) == d_row + 8 * g, R[:, g, f], 0.0)
        d_ref[0, f] = jnp.sum(tot, axis=1)


def tables(north, up, dens, thick, basin, lat_axis=None, lat_total=128, pairs=19, rounds=2):
    months, levels, rows, lons = north.shape
    groups = rows // 8
    npairs = pairs * rounds
    big = lambda: pl.BlockSpec((1, levels, rows, lons), lambda m: (m, 0, 0, 0))
    return pl.pallas_call(
        functools.partial(tables_kernel, lat_axis, lat_total, pairs, rounds),
        grid=(months,),
        in_specs=[big(), big(), big(),
                  pl.BlockSpec((levels, rows, lons), lambda m: (0, 0, 0), pipeline_mode=pl.Buffered(1)),
                  pl.BlockSpec((rows, lons), lambda m: (0, 0), pipeline_mode=pl.Buffered(1))],
        out_specs=[pl.BlockSpec((1, groups, 16, 256), lambda m: (m, 0, 0, 0)),
                   pl.BlockSpec((1, 2, npairs, 256), lambda m: (m, 0, 0, 0))],
        out_shape=[jax.ShapeDtypeStruct((months, groups, 16, 256), jnp.float32),
                   jax.ShapeDtypeStruct((months, 2, npairs, 256), jnp.float32)],
        scratch_shapes=[
            pltpu.VMEM((2 * npairs, rows, lons), jnp.float32),
            pltpu.VMEM((2 * npairs, rows, lons), jnp.float32),
            pltpu.VMEM((rows, lons), jnp.int32),
            pltpu.VMEM((256, 256), jnp.bfloat16),
            pltpu.VMEM((groups, 128, 256), jnp.float32),
            pltpu.VMEM((npairs, 16 * groups, 256), jnp.bfloat16),
        ],
        compiler_params=pltpu.CompilerParams(vmem_limit_bytes=60 * 2**20),
        name="tables",
    )(north, up, dens, thick, basin)


def merge_kernel(nlon, nlat, nmem, t_ref, d_ref, dm_ref, ds_ref, cm_ref, cs_ref,
                 tb, db, pk, pb, a_ref, mine, got, res,
                 send_l, recv_l, send_x, recv_x, send_m, recv_m, send_g, recv_g):
    f32 = jnp.float32
    mesh_id = pl.DeviceIdType.MESH
    y, x, me = lax.axis_index("lon"), lax.axis_index("lat"), lax.axis_index("mem")
    groups = t_ref.shape[1]
    lat_rows = 8 * groups
    piece = 320 // nmem

    def other(axis, index):
        return dict(device_id={axis: index}, device_id_type=mesh_id)

    barrier = pltpu.get_barrier_semaphore()
    for axis, at, n in (("lon", y, nlon), ("lat", x, nlat), ("mem", me, nmem)):
        for d in range(1, n):
            pl.semaphore_signal(barrier, inc=1, **other(axis, lax.rem(at + d, n)))
    pl.semaphore_wait(barrier, nlon + nlat + nmem - 3)

    sends = []
    for d in range(1, nlon):
        p = lax.rem(y + d, nlon)
        for q, (src, dst) in enumerate(((t_ref, tb), (d_ref, db))):
            c = pltpu.make_async_remote_copy(
                src.at[p], dst.at[d - 1], send_l.at[d - 1, q], recv_l.at[d - 1, q], **other("lon", p))
            c.start()
            sends.append(c)
    lane = lax.broadcasted_iota(jnp.int32, (8, 128), 1)
    wide = lax.broadcasted_iota(jnp.int32, (80, 128), 1)
    tall = lax.broadcasted_iota(jnp.int32, (80, 128), 0)

    def down(v):
        for s in (1, 2, 4, 8, 16, 32, 64):
            v = v + jnp.where(tall >= s, pltpu.roll(v, s, 0), 0.0)
        return v

    def along(v, at):
        s = 1
        while s < lat_rows:
            v = v + jnp.where(at % lat_rows >= s, pltpu.roll(v, s, 1), 0.0)
            s *= 2
        return v

    def regions(v):
        g = pltpu.roll(v, lat_rows, 1) + pltpu.roll(v, 2 * lat_rows, 1) + pltpu.roll(v, 3 * lat_rows, 1)
        return jnp.where((wide >= 3 * lat_rows) & (wide < 4 * lat_rows), g, v)

    for c in sends:
        c.wait_recv()
    T = t_ref[y]
    D = d_ref[y]
    for d in range(nlon - 1):
        T = T + tb[d]
        D = D + db[d]

    for f in range(2):
        R = {}
        for g in range(groups):
            for b in range(3):
                v = T[g, 5 * b:5 * b + 5, 128 * f:128 * f + 128]
                v = jnp.concatenate([v, jnp.zeros((3, 128), f32)], 0)
                s = lat_rows * b + 8 * g
                R[b, g] = pltpu.roll(v, s, 1) if s else v
        for l in range(16):
            z = jnp.zeros((8, 128), f32)
            for (b, g), v in R.items():
                z = jnp.where(lane // 8 == (groups * b + g + l) % 16, v, z)
            if l:
                z = pltpu.roll(z, 128 - 8 * l, 1)
            a_ref[f, pl.ds(l, 5, stride=16), :] = z[:5]
        levels2 = D.shape[1]
        a_ref[2 + f, 72:80, :] = jnp.zeros((8, 128), f32)
        a_ref[2 + f, pl.ds(0, levels2, stride=2), :] = D[f, :, 0:128]
        a_ref[2 + f, pl.ds(1, levels2, stride=2), :] = D[f, :, 128:256]

    up = [along(regions(a_ref[1]), wide), along(regions(a_ref[3]), wide)]
    packed = jnp.zeros((8, 128), f32)
    for q in range(2):
        for v in range(10):
            r = (10 * q + v - (lat_rows - 1)) % 128
            w = up[q][8 * v:8 * v + 8]
            packed = jnp.where(lane % lat_rows == 10 * q + v, pltpu.roll(w, r, 1) if r else w, packed)
    pk[...] = packed
    sends_x = []
    for d in range(1, nlat):
        p = lax.rem(x + d, nlat)
        c = pltpu.make_async_remote_copy(
            pk, pb.at[d - 1], send_x.at[d - 1], recv_x.at[d - 1], **other("lat", p))
        c.start()
        sends_x.append(c)

    def hand_in(a, v):
        a_ref[a] = v
        for o in range(a * nmem // 4, (a + 1) * nmem // 4):
            r0 = o * piece - 80 * a
            mine[o] = a_ref[a, r0:r0 + piece, :]

    hand_in(0, down(regions(a_ref[0])))
    hand_in(2, down(regions(a_ref[2])))

    carry = jnp.zeros((8, 128), f32)
    for d, c in enumerate(sends_x):
        c.wait_recv()
        carry = carry + jnp.where(x > d, pb[d], 0.0)
    for q in range(2):
        parts = []
        for v in range(10):
            r = (-(10 * q + v)) % 128
            w = pltpu.roll(carry, r, 1) if r else carry
            parts.append(jnp.where((lane % lat_rows == 0) & (lane < 4 * lat_rows), w, 0.0))
        up[q] = up[q] + along(jnp.concatenate(parts, 0), wide)
    hand_in(1, down(up[0]))
    hand_in(3, up[1])

    sends_m = []
    for d in range(1, nmem):
        p = lax.rem(me + d, nmem)
        c = pltpu.make_async_remote_copy(
            mine.at[p], got.at[d - 1], send_m.at[d - 1], recv_m.at[d - 1], **other("mem", p))
        c.start()
        sends_m.append(c)
    own = mine[me]
    total = own
    for d, c in enumerate(sends_m):
        c.wait_recv()
        total = total + got[d]
    mean = total * (1.0 / nmem)
    square = jnp.square(own - mean)
    for d in range(nmem - 1):
        square = square + jnp.square(got[d] - mean)
    res[me, 0] = mean
    res[me, 1] = jnp.sqrt(square * (1.0 / (nmem - 1)))

    core = lax.rem(me, 2)
    partner = me + 1 - 2 * core
    sends_g = []

    def give(piece_of, to, slot):
        c = pltpu.make_async_remote_copy(
            res.at[piece_of], res.at[piece_of], send_g.at[slot], recv_g.at[piece_of], **other("mem", to))
        c.start()
        sends_g.append(c)

    def take(piece_of):
        pltpu.make_async_remote_copy(
            res.at[piece_of], res.at[piece_of], send_g.at[0], recv_g.at[piece_of], **other("mem", partner)).wait_recv()

    for d in range(2, nmem, 2):
        give(me, lax.rem(me + d, nmem), d)
    give(me, partner, 0)
    for d in range(2, nmem, 2):
        p = lax.rem(me + nmem - d, nmem)
        take(p)
        give(p, partner, d + 1)
    for d in range(0, nmem, 2):
        take(lax.rem(partner + nmem - d, nmem))

    for k, (c_out, d_out) in enumerate(((cm_ref, dm_ref), (cs_ref, ds_ref))):
        for a, out in enumerate((c_out, c_out, d_out, d_out)):
            f = a % 2
            for o in range(a * nmem // 4, (a + 1) * nmem // 4):
                r0 = o * piece - 80 * a
                a_ref[a, r0:r0 + piece, :] = res[o, k]
            v = jnp.concatenate([a_ref[a], jnp.zeros((48, 128), f32)], 0).T
            n = out.shape[-1]
            for r in range(4):
                s = lat_rows * ((r + 3) % 4)
                out[0, r, f] = v[s:s + lat_rows, :n]
    for c in sends + sends_x + sends_m + sends_g:
        c.wait_send()


def merge(t, d, levels, nlon, nlat, nmem):
    f32 = jnp.float32
    groups = t.shape[1]
    lat_rows = 8 * groups
    piece = 320 // nmem
    vm = pl.BlockSpec(memory_space=pltpu.VMEM)
    sem = pltpu.SemaphoreType.DMA
    dep = jax.ShapeDtypeStruct((1, 4, 2, lat_rows, levels), f32)
    cla = jax.ShapeDtypeStruct((1, 4, 2, lat_rows, 80), f32)
    outs = pl.pallas_call(
        functools.partial(merge_kernel, nlon, nlat, nmem),
        in_specs=[vm, vm],
        out_specs=[vm] * 4,
        out_shape=[dep, dep, cla, cla],
        scratch_shapes=[
            pltpu.VMEM((nlon - 1, *t.shape[1:]), f32),
            pltpu.VMEM((nlon - 1, *d.shape[1:]), f32),
            pltpu.VMEM((8, 128), f32),
            pltpu.VMEM((nlat - 1, 8, 128), f32),
            pltpu.VMEM((4, 80, 128), f32),
            pltpu.VMEM((nmem, piece, 128), f32),
            pltpu.VMEM((nmem - 1, piece, 128), f32),
            pltpu.VMEM((nmem, 2, piece, 128), f32),
            sem((nlon - 1, 2)), sem((nlon - 1, 2)),
            sem((nlat - 1,)), sem((nlat - 1,)),
            sem((nmem - 1,)), sem((nmem - 1,)),
            sem((nmem + 1,)), sem((nmem,)),
        ],
        compiler_params=pltpu.CompilerParams(collective_id=0, has_side_effects=True),
        name="merge",
    )(t, d)
    return tuple(jnp.swapaxes(o, 3, 4) for o in outs)


def solution(mesh):
    nlon, nlat, nmem = (mesh.shape[a] for a in ("lon", "lat", "mem"))

    def body(north_vel, up_vel, dens_class, thickness, basin_id):
        t, d = tables(
            north_vel[0], up_vel[0], dens_class[0], thickness, basin_id,
            "lat", nlat * thickness.shape[1])
        return merge(t, d, thickness.shape[0], nlon, nlat, nmem)

    big = P("mem", None, None, "lat", "lon")
    out = P("lon", None, None, None, "lat")
    return jax.shard_map(
        body, mesh=mesh, in_specs=(big, big, big, P(None, "lat", "lon"), P("lat", "lon")),
        out_specs=(out,) * 4, check_vma=False)
```

```python
import functools
import math

import jax
import jax.numpy as jnp
from jax import lax
from jax.experimental import pallas as pl
from jax.experimental.pallas import tpu as pltpu
from jax.sharding import PartitionSpec as P

def tables_kernel(lat_axis, lat_total, pairs, rounds, n_ref, u_ref, c_ref, th_ref, b_ref, t_ref, d_ref,
                  cn_ref, cr_ref, hb_ref, mk_ref, f_ref):
    levels, rows, lons = th_ref.shape
    groups = rows // 8
    bf, f32, f8 = jnp.bfloat16, jnp.float32, jnp.float8_e4m3fn

    @pl.when(pl.program_id(0) == 0)
    def _():
        first = (lax.axis_index(lat_axis) if lat_axis else 0) * rows
        j = lax.broadcasted_iota(jnp.int32, (rows, lons), 0) + first
        phi = (-78.0 + 156.0 * (j.astype(f32) + 0.5) / lat_total) * (math.pi / 180.0)
        zw = jnp.cos(phi)

        @pl.loop(0, levels)
        def _(k):
            th = th_ref[k]
            cn_ref[k] = (0.02 * zw) * (th.astype(f32) * 0.001)
            cr_ref[k] = jnp.where(th > 0, 0.01 * zw, 0.0)

        for k in range(levels, cn_ref.shape[0]):
            cn_ref[k] = jnp.zeros((rows, lons), f32)
            cr_ref[k] = jnp.zeros((rows, lons), f32)
        b = b_ref[...]
        hb_ref[...] = jnp.where(b > 0, (b - 1) * 10, -100)
        z = jnp.zeros((128, lons), bf)
        m = jnp.concatenate([(b == v).astype(f32) for v in (1, 2, 3)] + [jnp.zeros((128 - 3 * rows, lons), f32)], 0).astype(bf)
        mk_ref[...] = jnp.concatenate(
            [jnp.concatenate([m, z], 1), jnp.concatenate([z, m], 1)], 0)

    zero = jnp.zeros((16, lons), bf)
    one = jnp.ones((16, lons), bf)

    def build(k, tile):
        kk = jnp.minimum(k, levels - 1)
        r0 = 16 * tile
        nf = n_ref[0, kk, r0:r0 + 16, :].astype(f32) * cn_ref[k, r0:r0 + 16, :]
        rf = u_ref[0, kk, r0:r0 + 16, :].astype(f32) * cr_ref[k, r0:r0 + 16, :]
        cc = c_ref[0, kk, r0:r0 + 16, :]
        hi = ((cc >> 3) + hb_ref[r0:r0 + 16, :]).astype(f32)
        lo = (cc & 7).astype(f32)
        out = []
        for s in range(2):
            a, b = nf[8 * s:8 * s + 8], rf[8 * s:8 * s + 8]
            h, l = hi[8 * s:8 * s + 8], lo[8 * s:8 * s + 8]
            nn = jnp.concatenate([a, a], 0).astype(bf)
            rr = jnp.concatenate([b, b], 0).astype(bf)
            fl = jnp.concatenate([a, b], 0).astype(bf)
            hh = jnp.concatenate([h, h - 1.0], 0).astype(bf)
            ll = jnp.concatenate([l, l - 1.0], 0).astype(bf)
            S = [jnp.where(hh == bf(2 * q), one, zero) for q in range(16)]
            S = [jnp.concatenate(S[2 * q:2 * q + 2], 0).astype(f8) for q in range(8)]
            ms = [ll == bf(2 * q) for q in range(4)]
            P = [jnp.where(m, nn, zero) for m in ms] + [jnp.where(m, rr, zero) for m in ms]
            out.append((jnp.concatenate(S, 0), jnp.concatenate(P, 0), fl))
        return out

    i_row = lax.broadcasted_iota(jnp.int32, (8, 256), 0)
    i_col = lax.broadcasted_iota(jnp.int32, (8, 256), 1)

    def month(accs, deps):
        @pl.loop(0, rounds)
        def _(r):
            for p in range(pairs):
                for tile in range(groups // 2):
                    even = build(2 * (r * pairs + p), tile)
                    odd = build(2 * (r * pairs + p) + 1, tile)
                    for s in range(2):
                        g = 2 * tile + s
                        S, P, F = (jnp.concatenate([x, y], 1) for x, y in zip(even[s], odd[s]))
                        pltpu.matmul_push_rhs(S, staging_register=tile % 2, mxu_index=s, transpose=True)
                        pltpu.matmul_acc_lhs(accs[g], P, load_staged_rhs=tile % 2)
                        f_ref[g, r * pairs + p] = F

        for s in range(2):
            pltpu.matmul_push_rhs(mk_ref[...], staging_register=0, mxu_index=s, transpose=True)
        half = f_ref.shape[1] // 2
        for h in range(2):
            tot = [0.0, 0.0]
            for g in range(groups):
                pltpu.matmul_acc_lhs(
                    deps[g], f_ref[g, half * h:half * h + half].reshape(16 * half, 256),
                    load_staged_rhs=0 if g < 2 and h == 0 else None)
            for g in range(groups):
                R = pltpu.matmul_pop(deps[g]).reshape(half, 2, 8, 256)
                for f in range(2):
                    tot[f] = tot[f] + jnp.where((i_col % rows) == i_row + 8 * g, R[:, f], 0.0)
            for f in range(2):
                d_ref[0, f, half * h:half * h + half, :] = jnp.sum(tot[f], axis=1)
        for g in range(groups):
            x = pltpu.matmul_pop(accs[g]).reshape(16, 8, 256)
            t_ref[0, g] = jnp.sum(jnp.where((i_col % 8) == i_row, x, 0.0), axis=1)

    half = f_ref.shape[1] // 2
    pl.run_scoped(
        month,
        tuple(pltpu.ACC(g % 2)((128, 256), f32) for g in range(groups)),
        tuple(pltpu.ACC(g % 2)((16 * half, 256), f32) for g in range(groups)))


def tables(north, up, dens, thick, basin, lat_axis=None, lat_total=128, pairs=19, rounds=2):
    months, levels, rows, lons = north.shape
    groups = rows // 8
    npairs = pairs * rounds
    big = lambda: pl.BlockSpec((1, levels, rows, lons), lambda m: (m, 0, 0, 0))
    return pl.pallas_call(
        functools.partial(tables_kernel, lat_axis, lat_total, pairs, rounds),
        grid=(months,),
        in_specs=[big(), big(), big(),
                  pl.BlockSpec((levels, rows, lons), lambda m: (0, 0, 0), pipeline_mode=pl.Buffered(1)),
                  pl.BlockSpec((rows, lons), lambda m: (0, 0), pipeline_mode=pl.Buffered(1))],
        out_specs=[pl.BlockSpec((1, groups, 16, 256), lambda m: (m, 0, 0, 0)),
                   pl.BlockSpec((1, 2, npairs, 256), lambda m: (m, 0, 0, 0))],
        out_shape=[jax.ShapeDtypeStruct((months, groups, 16, 256), jnp.float32),
                   jax.ShapeDtypeStruct((months, 2, npairs, 256), jnp.float32)],
        scratch_shapes=[
            pltpu.VMEM((2 * npairs, rows, lons), jnp.float32),
            pltpu.VMEM((2 * npairs, rows, lons), jnp.float32),
            pltpu.VMEM((rows, lons), jnp.int32),
            pltpu.VMEM((256, 256), jnp.bfloat16),
            pltpu.VMEM((groups, npairs, 16, 256), jnp.bfloat16),
        ],
        compiler_params=pltpu.CompilerParams(vmem_limit_bytes=60 * 2**20),
        name="tables",
    )(north, up, dens, thick, basin)


def merge_kernel(nlon, nlat, nmem, t_ref, d_ref, all_ref,
                 tb, db, pk, pb, a_ref, mine, got, res,
                 send_l, recv_l, send_x, recv_x, send_m, recv_m, send_g, recv_g):
    f32 = jnp.float32
    mesh_id = pl.DeviceIdType.MESH
    y, x, me = lax.axis_index("lon"), lax.axis_index("lat"), lax.axis_index("mem")
    groups = t_ref.shape[1]
    lat_rows = 8 * groups
    piece = 320 // nmem

    def other(axis, index):
        return dict(device_id={axis: index}, device_id_type=mesh_id)

    barrier = pltpu.get_barrier_semaphore()
    for axis, at, n in (("lon", y, nlon), ("lat", x, nlat), ("mem", me, nmem)):
        for d in range(1, n):
            pl.semaphore_signal(barrier, inc=1, **other(axis, lax.rem(at + d, n)))
    pl.semaphore_wait(barrier, nlon + nlat + nmem - 3)

    sends = []
    for d in range(1, nlon):
        p = lax.rem(y + d, nlon)
        for q, (src, dst) in enumerate(((t_ref, tb), (d_ref, db))):
            c = pltpu.make_async_remote_copy(
                src.at[p], dst.at[d - 1], send_l.at[d - 1, q], recv_l.at[d - 1, q], **other("lon", p))
            c.start()
            sends.append(c)
    lane = lax.broadcasted_iota(jnp.int32, (8, 128), 1)
    wide = lax.broadcasted_iota(jnp.int32, (80, 128), 1)
    tall = lax.broadcasted_iota(jnp.int32, (80, 128), 0)

    def down(v):
        for s in (1, 2, 4, 8, 16, 32, 64):
            v = v + jnp.where(tall >= s, pltpu.roll(v, s, 0), 0.0)
        return v

    def along(v, at):
        s = 1
        while s < lat_rows:
            v = v + jnp.where(at % lat_rows >= s, pltpu.roll(v, s, 1), 0.0)
            s *= 2
        return v

    def regions(v):
        g = pltpu.roll(v, lat_rows, 1) + pltpu.roll(v, 2 * lat_rows, 1) + pltpu.roll(v, 3 * lat_rows, 1)
        return jnp.where((wide >= 3 * lat_rows) & (wide < 4 * lat_rows), g, v)

    for c in sends:
        c.wait_recv()
    T = t_ref[y]
    D = d_ref[y]
    for d in range(nlon - 1):
        T = T + tb[d]
        D = D + db[d]

    for f in range(2):
        R = {}
        for g in range(groups):
            for b in range(3):
                v = T[g, 8 * f:8 * f + 8, :]
                s = (lat_rows * b + 8 * g - 80 * b) % 256
                R[b, g] = pltpu.roll(v, s, 1) if s else v
        for h in range(10):
            z = jnp.zeros((8, 128), f32)
            for (b, g), v in R.items():
                q = groups * b + g + h
                z = jnp.where(lane // 8 == q % 16, v[:, :128] if q < 16 else v[:, 128:], z)
            if h:
                z = pltpu.roll(z, 128 - 8 * h, 1)
            a_ref[f, 8 * h:8 * h + 8, :] = z
        levels2 = D.shape[1]
        a_ref[2 + f, 72:80, :] = jnp.zeros((8, 128), f32)
        a_ref[2 + f, pl.ds(0, levels2, stride=2), :] = D[f, :, 0:128]
        a_ref[2 + f, pl.ds(1, levels2, stride=2), :] = D[f, :, 128:256]

    up = [along(regions(a_ref[1]), wide), along(regions(a_ref[3]), wide)]
    packed = jnp.zeros((8, 128), f32)
    for q in range(2):
        for v in range(10):
            r = (10 * q + v - (lat_rows - 1)) % 128
            w = up[q][8 * v:8 * v + 8]
            packed = jnp.where(lane % lat_rows == 10 * q + v, pltpu.roll(w, r, 1) if r else w, packed)
    pk[...] = packed
    sends_x = []
    for d in range(1, nlat):
        p = lax.rem(x + d, nlat)
        c = pltpu.make_async_remote_copy(
            pk, pb.at[d - 1], send_x.at[d - 1], recv_x.at[d - 1], **other("lat", p))
        c.start()
        sends_x.append(c)

    def hand_in(a, v):
        a_ref[a] = v
        for o in range(a * nmem // 4, (a + 1) * nmem // 4):
            r0 = o * piece - 80 * a
            mine[o] = a_ref[a, r0:r0 + piece, :]

    hand_in(0, down(regions(a_ref[0])))
    hand_in(2, down(regions(a_ref[2])))

    carry = jnp.zeros((8, 128), f32)
    for d, c in enumerate(sends_x):
        c.wait_recv()
        carry = carry + jnp.where(x > d, pb[d], 0.0)
    for q in range(2):
        parts = []
        for v in range(10):
            r = (-(10 * q + v)) % 128
            w = pltpu.roll(carry, r, 1) if r else carry
            parts.append(jnp.where((lane % lat_rows == 0) & (lane < 4 * lat_rows), w, 0.0))
        up[q] = up[q] + along(jnp.concatenate(parts, 0), wide)
    hand_in(1, down(up[0]))
    hand_in(3, up[1])

    sends_m = []
    for d in range(1, nmem):
        p = lax.rem(me + d, nmem)
        c = pltpu.make_async_remote_copy(
            mine.at[p], got.at[d - 1], send_m.at[d - 1], recv_m.at[d - 1], **other("mem", p))
        c.start()
        sends_m.append(c)
    own = mine[me]
    total = own
    for d, c in enumerate(sends_m):
        c.wait_recv()
        total = total + got[d]
    mean = total * (1.0 / nmem)
    square = jnp.square(own - mean)
    for d in range(nmem - 1):
        square = square + jnp.square(got[d] - mean)
    res[me, 0] = mean
    res[me, 1] = jnp.sqrt(square * (1.0 / (nmem - 1)))

    core = lax.rem(me, 2)
    partner = me + 1 - 2 * core
    sends_g = []

    def give(piece_of, to, slot):
        c = pltpu.make_async_remote_copy(
            res.at[piece_of], res.at[piece_of], send_g.at[slot], recv_g.at[piece_of], **other("mem", to))
        c.start()
        sends_g.append(c)

    def take(piece_of):
        pltpu.make_async_remote_copy(
            res.at[piece_of], res.at[piece_of], send_g.at[0], recv_g.at[piece_of], **other("mem", partner)).wait_recv()

    for d in range(2, nmem, 2):
        give(me, lax.rem(me + d, nmem), d)
    give(me, partner, 0)
    for d in range(2, nmem, 2):
        p = lax.rem(me + nmem - d, nmem)
        take(p)
        give(p, partner, d + 1)
    for d in range(0, nmem, 2):
        take(lax.rem(partner + nmem - d, nmem))

    all_ref[...] = res[...]
    for c in sends + sends_x + sends_m + sends_g:
        c.wait_send()


def merge(t, d, nlon, nlat, nmem):
    f32 = jnp.float32
    groups = t.shape[1]
    lat_rows = 8 * groups
    piece = 320 // nmem
    vm = pl.BlockSpec(memory_space=pltpu.VMEM)
    sem = pltpu.SemaphoreType.DMA
    return pl.pallas_call(
        functools.partial(merge_kernel, nlon, nlat, nmem),
        in_specs=[vm, vm],
        out_specs=vm,
        out_shape=jax.ShapeDtypeStruct((nmem, 2, piece, 128), f32),
        scratch_shapes=[
            pltpu.VMEM((nlon - 1, *t.shape[1:]), f32),
            pltpu.VMEM((nlon - 1, *d.shape[1:]), f32),
            pltpu.VMEM((8, 128), f32),
            pltpu.VMEM((nlat - 1, 8, 128), f32),
            pltpu.VMEM((4, 80, 128), f32),
            pltpu.VMEM((nmem, piece, 128), f32),
            pltpu.VMEM((nmem - 1, piece, 128), f32),
            pltpu.VMEM((nmem, 2, piece, 128), f32),
            sem((nlon - 1, 2)), sem((nlon - 1, 2)),
            sem((nlat - 1,)), sem((nlat - 1,)),
            sem((nmem - 1,)), sem((nmem - 1,)),
            sem((nmem + 1,)), sem((nmem,)),
        ],
        compiler_params=pltpu.CompilerParams(collective_id=0, has_side_effects=True),
        name="merge",
    )(t, d)


def finish_kernel(lat_rows, all_ref, dm_ref, ds_ref, cm_ref, cs_ref, a_ref):
    nmem, piece = all_ref.shape[0], all_ref.shape[2]
    a_ref[...] = jnp.zeros_like(a_ref)
    for k, outs in enumerate(((cm_ref, dm_ref), (cs_ref, ds_ref))):
        for a in range(4):
            for o in range(a * nmem // 4, (a + 1) * nmem // 4):
                r0 = o * piece - 80 * a
                a_ref[4 * k + a, r0:r0 + piece, :] = all_ref[o, k]
        for a in range(4):
            v = a_ref[4 * k + a].T
            out = outs[a // 2]
            for r in range(4):
                s = lat_rows * ((r + 3) % 4)
                out[0, r, a % 2] = v[s:s + lat_rows, :out.shape[-1]]


def finish(res, levels, lat_rows):
    f32 = jnp.float32
    vm = pl.BlockSpec(memory_space=pltpu.VMEM)
    dep = jax.ShapeDtypeStruct((1, 4, 2, lat_rows, levels), f32)
    cla = jax.ShapeDtypeStruct((1, 4, 2, lat_rows, 80), f32)
    outs = pl.pallas_call(
        functools.partial(finish_kernel, lat_rows),
        in_specs=[vm],
        out_specs=[vm] * 4,
        out_shape=[dep, dep, cla, cla],
        scratch_shapes=[pltpu.VMEM((8, 128, 128), f32)],
        name="finish",
    )(res)
    return tuple(jnp.swapaxes(o, 3, 4) for o in outs)


def solution(mesh):
    nlon, nlat, nmem = (mesh.shape[a] for a in ("lon", "lat", "mem"))

    def body(north_vel, up_vel, dens_class, thickness, basin_id):
        t, d = tables(
            north_vel[0], up_vel[0], dens_class[0], thickness, basin_id,
            "lat", nlat * thickness.shape[1])
        res = merge(t, d, nlon, nlat, nmem)
        return finish(res, *thickness.shape[:2])

    big = P("mem", None, None, "lat", "lon")
    out = P("lon", None, None, None, "lat")
    return jax.shard_map(
        body, mesh=mesh, in_specs=(big, big, big, P(None, "lat", "lon"), P("lat", "lon")),
        out_specs=(out,) * 4, check_vma=False)
```

```python
import functools
import math

import jax
import jax.numpy as jnp
from jax import lax
from jax.experimental import pallas as pl
from jax.experimental.pallas import tpu as pltpu
from jax.sharding import PartitionSpec as P

MESH = pl.DeviceIdType.MESH
PIECE = 320
UNROLL = 19


def build(n_ref, u_ref, c_ref, cn_ref, cr_ref, hb_ref, slot, k, tile):
    bf, f32, f8 = jnp.bfloat16, jnp.float32, jnp.float8_e4m3fn
    r0 = 16 * tile
    nf = n_ref[slot, k, r0:r0 + 16, :].astype(f32) * cn_ref[k, r0:r0 + 16, :]
    rf = u_ref[slot, k, r0:r0 + 16, :].astype(f32) * cr_ref[k, r0:r0 + 16, :]
    cc = c_ref[slot, k, r0:r0 + 16, :]
    hi = ((cc >> 3) + hb_ref[r0:r0 + 16, :]).astype(f32)
    lo = (cc & 7).astype(f32)
    zero = jnp.zeros((16, cc.shape[1]), bf)
    one = jnp.ones((16, cc.shape[1]), bf)
    out = []
    for s in range(2):
        a, b = nf[8 * s:8 * s + 8], rf[8 * s:8 * s + 8]
        h, l = hi[8 * s:8 * s + 8], lo[8 * s:8 * s + 8]
        nn = jnp.concatenate([a, a], 0).astype(bf)
        rr = jnp.concatenate([b, b], 0).astype(bf)
        fl = jnp.concatenate([a, b], 0).astype(bf)
        hh = jnp.concatenate([h, h - 1.0], 0).astype(bf)
        ll = jnp.concatenate([l, l - 1.0], 0).astype(bf)
        S = [jnp.where(hh == bf(2 * q), one, zero) for q in range(16)]
        S = [jnp.concatenate(S[2 * q:2 * q + 2], 0).astype(f8) for q in range(8)]
        ms = [ll == bf(2 * q) for q in range(4)]
        V = [jnp.where(m, nn, zero) for m in ms] + [jnp.where(m, rr, zero) for m in ms]
        out.append((jnp.concatenate(S, 0), jnp.concatenate(V, 0), fl))
    return out


def kernel(nlon, nlat, nmem, n_hbm, u_hbm, c_hbm, th_hbm, b_ref, all_ref,
           n_buf, u_buf, c_buf, th_ref, cn_ref, cr_ref, hb_ref, mk_ref, f_ref,
           t_ref, d_ref, tb, db, pk, pb, a_ref, mine, got, res,
           in_sem, th_sem, send_l, recv_l, send_x, recv_x, send_m, recv_m, send_g, recv_g):
    bf, f32 = jnp.bfloat16, jnp.float32
    y, x, me = lax.axis_index("lon"), lax.axis_index("lat"), lax.axis_index("mem")
    months, levels, rows, lons = n_hbm.shape
    groups = rows // 8
    padded = cn_ref.shape[0]
    npairs = padded // 2
    half = npairs // 2
    rounds = npairs // UNROLL
    nz = nmem // 2
    piece = PIECE // nmem

    def other(axis, index):
        return dict(device_id={axis: index}, device_id_type=MESH)

    barrier = pltpu.get_barrier_semaphore()
    for axis, at, n in (("lon", y, nlon), ("lat", x, nlat), ("mem", me, nmem)):
        for d in range(1, n):
            pl.semaphore_signal(barrier, inc=1, **other(axis, lax.rem(at + d, n)))

    def inputs(s):
        month, slot = lax.rem(y + 1 + s, months), lax.rem(s, 2)
        return [pltpu.make_async_copy(src.at[month], buf.at[slot, pl.ds(0, levels)], in_sem.at[slot, q])
                for q, (src, buf) in enumerate(((n_hbm, n_buf), (u_hbm, u_buf), (c_hbm, c_buf)))]

    th_copy = pltpu.make_async_copy(th_hbm, th_ref, th_sem)
    th_copy.start()
    for c in inputs(0):
        c.start()
    for slot in range(2):
        for k in range(levels, padded):
            n_buf[slot, k] = jnp.zeros((rows, lons), bf)
            u_buf[slot, k] = jnp.zeros((rows, lons), bf)
            c_buf[slot, k] = jnp.zeros((rows, lons), jnp.int32)
    for k in range(levels, padded):
        cn_ref[k] = jnp.zeros((rows, lons), f32)
        cr_ref[k] = jnp.zeros((rows, lons), f32)
    b = b_ref[...]
    hb_ref[...] = jnp.where(b > 0, (b - 1) * 10, -100)
    z = jnp.zeros((128, lons), bf)
    m = jnp.concatenate([(b == v).astype(f32) for v in (1, 2, 3)]
                        + [jnp.zeros((128 - 3 * rows, lons), f32)], 0).astype(bf)
    mk_ref[...] = jnp.concatenate([jnp.concatenate([m, z], 1), jnp.concatenate([z, m], 1)], 0)
    j = lax.broadcasted_iota(jnp.int32, (rows, lons), 0) + x * rows
    phi = (-78.0 + 156.0 * (j.astype(f32) + 0.5) / (rows * nlat)) * (math.pi / 180.0)
    zw = jnp.cos(phi)
    zn, zr = 0.02 * zw, 0.01 * zw
    th_copy.wait()

    @pl.loop(0, levels // 5)
    def _(q):
        for k in range(5):
            th = th_ref[5 * q + k]
            cn_ref[5 * q + k] = zn * (th.astype(f32) * 0.001)
            cr_ref[5 * q + k] = jnp.where(th > 0, zr, 0.0)

    for k in range(levels // 5 * 5, levels):
        th = th_ref[k]
        cn_ref[k] = zn * (th.astype(f32) * 0.001)
        cr_ref[k] = jnp.where(th > 0, zr, 0.0)

    i_row = lax.broadcasted_iota(jnp.int32, (8, 256), 0)
    i_col = lax.broadcasted_iota(jnp.int32, (8, 256), 1)

    def to_owner(s):
        p = lax.rem(y + 1 + s, nlon)
        return [pltpu.make_async_remote_copy(
            src.at[s], dst.at[s], send_l.at[s, q], recv_l.at[s, q], **other("lon", p))
            for q, (src, dst) in enumerate(((t_ref, tb), (d_ref, db)))]

    def tables(accs, deps):
        @pl.loop(0, months)
        def _(s):
            slot = lax.rem(s, 2)
            for c in inputs(s):
                c.wait()

            @pl.when(s < months - 1)
            def _():
                for c in inputs(s + 1):
                    c.start()

            @pl.loop(0, rounds)
            def _(r):
                for p in range(UNROLL):
                    for tile in range(groups // 2):
                        even, odd = (build(n_buf, u_buf, c_buf, cn_ref, cr_ref, hb_ref,
                                           slot, 2 * (r * UNROLL + p) + e, tile) for e in range(2))
                        for q in range(2):
                            g = 2 * tile + q
                            S, V, F = (jnp.concatenate([v, w], 1) for v, w in zip(even[q], odd[q]))
                            pltpu.matmul_push_rhs(S, staging_register=tile % 2, mxu_index=q, transpose=True)
                            pltpu.matmul_acc_lhs(accs[g], V, load_staged_rhs=tile % 2)
                            f_ref[g, r * UNROLL + p] = F

            for q in range(2):
                pltpu.matmul_push_rhs(mk_ref[...], staging_register=0, mxu_index=q, transpose=True)
            for g in range(groups):
                v = pltpu.matmul_pop(accs[g]).reshape(16, 8, 256)
                t_ref[s, g] = jnp.sum(jnp.where((i_col % 8) == i_row, v, 0.0), axis=1)
            for h in range(2):
                tot = [0.0, 0.0]
                for g in range(groups):
                    pltpu.matmul_acc_lhs(
                        deps[g], f_ref[g, half * h:half * h + half].reshape(16 * half, 256),
                        load_staged_rhs=0 if g < 2 and h == 0 else None)
                for g in range(groups):
                    R = pltpu.matmul_pop(deps[g]).reshape(half, 2, 8, 256)
                    for f in range(2):
                        tot[f] = tot[f] + jnp.where((i_col % rows) == i_row + 8 * g, R[:, f], 0.0)
                for f in range(2):
                    d_ref[s, f, half * h:half * h + half, :] = jnp.sum(tot[f], axis=1)

            @pl.when(s == 0)
            def _():
                pl.semaphore_wait(barrier, nlon + nlat + nmem - 3)

            @pl.when(s < months - 1)
            def _():
                for c in to_owner(s):
                    c.start()

    pl.run_scoped(
        tables,
        tuple(pltpu.ACC(g % 2)((128, 256), f32) for g in range(groups)),
        tuple(pltpu.ACC(g % 2)((16 * half, 256), f32) for g in range(groups)))

    lane = lax.broadcasted_iota(jnp.int32, (8, 128), 1)
    wide = lax.broadcasted_iota(jnp.int32, (80, 128), 1)
    tall = lax.broadcasted_iota(jnp.int32, (80, 128), 0)

    def down(v):
        for s in (1, 2, 4, 8, 16, 32, 64):
            v = v + jnp.where(tall >= s, pltpu.roll(v, s, 0), 0.0)
        return v

    def along(v):
        s = 1
        while s < rows:
            v = v + jnp.where(wide % rows >= s, pltpu.roll(v, s, 1), 0.0)
            s *= 2
        return v

    def regions(v):
        w = pltpu.roll(v, rows, 1) + pltpu.roll(v, 2 * rows, 1) + pltpu.roll(v, 3 * rows, 1)
        return jnp.where((wide >= 3 * rows) & (wide < 4 * rows), w, v)

    sends_l = [c for s in range(months - 1) for c in to_owner(s)]
    for c in sends_l:
        c.wait_recv()

    def class_rows(f):
        R = {}
        for g in range(groups):
            T = t_ref[months - 1, g, 8 * f:8 * f + 8, :]
            for d in range(months - 1):
                T = T + tb[d, g, 8 * f:8 * f + 8, :]
            for q in range(3):
                s = (rows * q + 8 * g - 80 * q) % 256
                R[q, g] = pltpu.roll(T, s, 1) if s else T
        for h in range(10):
            z = jnp.zeros((8, 128), f32)
            for (q, g), v in R.items():
                o = groups * q + g + h
                z = jnp.where(lane // 8 == o % 16, v[:, :128] if o < 16 else v[:, 128:], z)
            a_ref[f, 8 * h:8 * h + 8, :] = pltpu.roll(z, 128 - 8 * h, 1) if h else z
        return regions(a_ref[f])

    def depth_rows(f):
        D = d_ref[months - 1, f]
        for d in range(months - 1):
            D = D + db[d, f]
        a_ref[2 + f, 72:80, :] = jnp.zeros((8, 128), f32)
        a_ref[2 + f, pl.ds(0, npairs, stride=2), :] = D[:, 0:128]
        a_ref[2 + f, pl.ds(1, npairs, stride=2), :] = D[:, 128:256]
        return regions(a_ref[2 + f])

    up = [along(class_rows(1)), along(depth_rows(1))]
    packed = jnp.zeros((8, 128), f32)
    for q in range(2):
        for v in range(10):
            r = (10 * q + v - (rows - 1)) % 128
            w = up[q][8 * v:8 * v + 8]
            packed = jnp.where(lane % rows == 10 * q + v, pltpu.roll(w, r, 1) if r else w, packed)
    pk[...] = packed
    sends_x = []
    for d in range(1, nlat):
        c = pltpu.make_async_remote_copy(
            pk, pb.at[d - 1], send_x.at[d - 1], recv_x.at[d - 1], **other("lat", lax.rem(x + d, nlat)))
        c.start()
        sends_x.append(c)

    core = lax.rem(me, 2)
    zz = (me - core) // 2
    far_first = sorted(range(1, nz), key=lambda d: (-min(d, nz - d), d))
    sends_m = []

    def piece_to(f, dz):
        to = 2 * lax.rem(zz + dz, nz) + f
        d = lax.rem(to - me + nmem, nmem)
        return pltpu.make_async_remote_copy(
            mine.at[to], got.at[d - 1], send_m.at[d - 1], recv_m.at[d - 1], **other("mem", to))

    def hand_in(f, tables_f):
        for q, v in enumerate(tables_f):
            a_ref[2 * q + f] = v
            for t in range(nz // 2):
                mine[2 * (q * (nz // 2) + t) + f] = a_ref[2 * q + f, piece * t:piece * t + piece, :]
        for dz in far_first:
            c = piece_to(f, dz)
            c.start()
            sends_m.append(c)

        @pl.when(core != f)
        def _():
            piece_to(f, 0).start()

    hand_in(0, [down(class_rows(0)), down(depth_rows(0))])

    carry = jnp.zeros((8, 128), f32)
    for d, c in enumerate(sends_x):
        c.wait_recv()
        carry = carry + jnp.where(x > d, pb[d], 0.0)
    for q in range(2):
        parts = []
        for v in range(10):
            r = (-(10 * q + v)) % 128
            w = pltpu.roll(carry, r, 1) if r else carry
            parts.append(jnp.where((lane % rows == 0) & (lane < 4 * rows), w, 0.0))
        up[q] = up[q] + along(jnp.concatenate(parts, 0))
    hand_in(1, [down(up[0]), up[1]])

    own = mine[me]
    total = own
    for d in range(1, nmem):
        pltpu.make_async_remote_copy(
            mine.at[me], got.at[d - 1], send_m.at[d - 1], recv_m.at[d - 1],
            **other("mem", lax.rem(me + d, nmem))).wait_recv()
        total = total + got[d - 1]
    mean = total * (1.0 / nmem)
    square = jnp.square(own - mean)
    for d in range(nmem - 1):
        square = square + jnp.square(got[d] - mean)
    res[me, 0] = mean
    res[me, 1] = jnp.sqrt(square * (1.0 / (nmem - 1)))

    partner = me + 1 - 2 * core
    sends_g = []

    def give(piece_of, to, slot):
        c = pltpu.make_async_remote_copy(
            res.at[piece_of], res.at[piece_of], send_g.at[slot], recv_g.at[piece_of], **other("mem", to))
        c.start()
        sends_g.append(c)

    def take(piece_of):
        pltpu.make_async_remote_copy(
            res.at[piece_of], res.at[piece_of], send_g.at[0], recv_g.at[piece_of], **other("mem", partner)).wait_recv()

    for dz in far_first:
        give(me, lax.rem(me + 2 * dz, nmem), 2 * dz)
    give(me, partner, 0)
    for dz in reversed(far_first):
        p = lax.rem(me + nmem - 2 * dz, nmem)
        take(p)
        give(p, partner, 2 * dz + 1)
    take(partner)
    for dz in reversed(far_first):
        take(lax.rem(partner + nmem - 2 * dz, nmem))

    all_ref[...] = res[...]
    for c in sends_l + sends_x + sends_g:
        c.wait_send()
    for d in range(1, nmem):
        pltpu.make_async_remote_copy(
            mine.at[me], got.at[d - 1], send_m.at[d - 1], recv_m.at[d - 1],
            **other("mem", lax.rem(me + d, nmem))).wait_send()


def statistics(north, up, dens, thick, basin, nlon, nlat, nmem):
    f32, bf, i32 = jnp.float32, jnp.bfloat16, jnp.int32
    months, levels, rows, lons = north.shape
    groups = rows // 8
    npairs = UNROLL * -(-levels // (2 * UNROLL))
    padded = 2 * npairs
    piece = PIECE // nmem
    vm = pl.BlockSpec(memory_space=pltpu.VMEM)
    hbm = pl.BlockSpec(memory_space=pl.ANY)
    sem = pltpu.SemaphoreType.DMA
    return pl.pallas_call(
        functools.partial(kernel, nlon, nlat, nmem),
        in_specs=[hbm, hbm, hbm, hbm, vm],
        out_specs=vm,
        out_shape=jax.ShapeDtypeStruct((nmem, 2, piece, 128), f32),
        scratch_shapes=[
            pltpu.VMEM((2, padded, rows, lons), bf),
            pltpu.VMEM((2, padded, rows, lons), bf),
            pltpu.VMEM((2, padded, rows, lons), i32),
            pltpu.VMEM((levels, rows, lons), i32),
            pltpu.VMEM((padded, rows, lons), f32),
            pltpu.VMEM((padded, rows, lons), f32),
            pltpu.VMEM((rows, lons), i32),
            pltpu.VMEM((256, 256), bf),
            pltpu.VMEM((groups, npairs, 16, 256), bf),
            pltpu.VMEM((months, groups, 16, 256), f32),
            pltpu.VMEM((months, 2, npairs, 256), f32),
            pltpu.VMEM((months - 1, groups, 16, 256), f32),
            pltpu.VMEM((months - 1, 2, npairs, 256), f32),
            pltpu.VMEM((8, 128), f32),
            pltpu.VMEM((nlat - 1, 8, 128), f32),
            pltpu.VMEM((4, 80, 128), f32),
            pltpu.VMEM((nmem, piece, 128), f32),
            pltpu.VMEM((nmem - 1, piece, 128), f32),
            pltpu.VMEM((nmem, 2, piece, 128), f32),
            sem((2, 3)), sem,
            sem((months - 1, 2)), sem((months - 1, 2)),
            sem((nlat - 1,)), sem((nlat - 1,)),
            sem((nmem - 1,)), sem((nmem - 1,)),
            sem((nmem,)), sem((nmem,)),
        ],
        compiler_params=pltpu.CompilerParams(
            collective_id=0, has_side_effects=True, vmem_limit_bytes=63 * 2**20),
        name="statistics",
    )(north, up, dens, thick, basin)


def finish_kernel(rows, all_ref, dm_ref, ds_ref, cm_ref, cs_ref, a_ref):
    nmem, piece = all_ref.shape[0], all_ref.shape[2]
    share = nmem // 4
    a_ref[...] = jnp.zeros_like(a_ref)
    for k, outs in enumerate(((cm_ref, dm_ref), (cs_ref, ds_ref))):
        for a in range(4):
            for t in range(share):
                o = 2 * (a // 2 * share + t) + a % 2
                a_ref[4 * k + a, piece * t:piece * t + piece, :] = all_ref[o, k]
        for a in range(4):
            v = a_ref[4 * k + a].T
            out = outs[a // 2]
            for r in range(4):
                s = rows * ((r + 3) % 4)
                out[0, r, a % 2] = v[s:s + rows, :out.shape[-1]]


def finish(res, levels, rows):
    f32 = jnp.float32
    vm = pl.BlockSpec(memory_space=pltpu.VMEM)
    dep = jax.ShapeDtypeStruct((1, 4, 2, rows, levels), f32)
    cla = jax.ShapeDtypeStruct((1, 4, 2, rows, 80), f32)
    outs = pl.pallas_call(
        functools.partial(finish_kernel, rows),
        in_specs=[vm],
        out_specs=[vm] * 4,
        out_shape=[dep, dep, cla, cla],
        scratch_shapes=[pltpu.VMEM((8, 128, 128), f32)],
        name="finish",
    )(res)
    return tuple(jnp.swapaxes(o, 3, 4) for o in outs)


def solution(mesh):
    nlon, nlat, nmem = (mesh.shape[a] for a in ("lon", "lat", "mem"))

    def body(north_vel, up_vel, dens_class, thickness, basin_id):
        res = statistics(north_vel[0], up_vel[0], dens_class[0], thickness, basin_id, nlon, nlat, nmem)
        return finish(res, *thickness.shape[:2])

    big = P("mem", None, None, "lat", "lon")
    out = P("lon", None, None, None, "lat")
    return jax.shard_map(
        body, mesh=mesh, in_specs=(big, big, big, P(None, "lat", "lon"), P("lat", "lon")),
        out_specs=(out,) * 4, check_vma=False)
```

```python
import functools
import math

import jax
import jax.numpy as jnp
from jax import lax
from jax.experimental import pallas as pl
from jax.experimental.pallas import tpu as pltpu
from jax.sharding import PartitionSpec as P

MESH = pl.DeviceIdType.MESH
UNROLL = 19


def build(n_ref, u_ref, c_ref, cn_ref, cr_ref, hb_ref, slot, k, tile):
    bf, f32, f8 = jnp.bfloat16, jnp.float32, jnp.float8_e4m3fn
    r0 = 16 * tile
    nf = n_ref[slot, k, r0:r0 + 16, :].astype(f32) * cn_ref[k, r0:r0 + 16, :]
    rf = u_ref[slot, k, r0:r0 + 16, :].astype(f32) * cr_ref[k, r0:r0 + 16, :]
    cc = c_ref[slot, k, r0:r0 + 16, :]
    hi = ((cc >> 3) + hb_ref[r0:r0 + 16, :]).astype(f32)
    lo = (cc & 7).astype(f32)
    zero = jnp.zeros((16, cc.shape[1]), bf)
    one = jnp.ones((16, cc.shape[1]), bf)
    out = []
    for s in range(2):
        a, b = nf[8 * s:8 * s + 8], rf[8 * s:8 * s + 8]
        h, l = hi[8 * s:8 * s + 8], lo[8 * s:8 * s + 8]
        nn = jnp.concatenate([a, a], 0).astype(bf)
        rr = jnp.concatenate([b, b], 0).astype(bf)
        fl = jnp.concatenate([a, b], 0).astype(bf)
        hh = jnp.concatenate([h, h - 1.0], 0).astype(bf)
        ll = jnp.concatenate([l, l - 1.0], 0).astype(bf)
        S = [jnp.where(hh == bf(2 * q), one, zero) for q in range(16)]
        S = [jnp.concatenate(S[2 * q:2 * q + 2], 0).astype(f8) for q in range(8)]
        ms = [ll == bf(2 * q) for q in range(4)]
        V = [jnp.where(m, nn, zero) for m in ms] + [jnp.where(m, rr, zero) for m in ms]
        out.append((jnp.concatenate(S, 0), jnp.concatenate(V, 0), fl))
    return out


def kernel(nlon, nlat, nmem, n_hbm, u_hbm, c_hbm, th_hbm, b_ref, all_ref,
           n_buf, u_buf, c_buf, th_ref, cn_ref, cr_ref, hb_ref, mk_ref, f_ref,
           t_ref, d_ref, tb, db, pk, pb, a_ref, mine, got, all_m, cs, cb, res,
           in_sem, th_sem, send_l, recv_l, send_x, recv_x, send_m, recv_m, send_c, recv_c, send_g, recv_g):
    bf, f32 = jnp.bfloat16, jnp.float32
    y, x, me = lax.axis_index("lon"), lax.axis_index("lat"), lax.axis_index("mem")
    months, levels, rows, lons = n_hbm.shape
    groups = rows // 8
    padded = cn_ref.shape[0]
    npairs = padded // 2
    half = npairs // 2
    rounds = npairs // UNROLL
    nz = nmem // 2
    per = 80 // nz
    piece = 2 * per

    def other(axis, index):
        return dict(device_id={axis: index}, device_id_type=MESH)

    chunk = 2 * UNROLL
    chunks = [(r, chunk * r, min(chunk, levels - chunk * r)) for r in range(rounds)]

    def inputs(s, r, k0, n):
        month, slot = lax.rem(y + 1 + s, months), lax.rem(s, 2)
        return [pltpu.make_async_copy(
            src.at[month, pl.ds(k0, n)], buf.at[slot, pl.ds(k0, n)], in_sem.at[slot, r, q])
            for q, (src, buf) in enumerate(((n_hbm, n_buf), (u_hbm, u_buf), (c_hbm, c_buf)))]

    def thick(r, k0, n):
        return pltpu.make_async_copy(th_hbm.at[pl.ds(k0, n)], th_ref.at[pl.ds(k0, n)], th_sem.at[r])

    for at in chunks:
        thick(*at).start()
        for c in inputs(0, *at):
            c.start()
    barrier = pltpu.get_barrier_semaphore()
    for axis, at, n in (("lon", y, nlon), ("lat", x, nlat), ("mem", me, nmem)):
        for d in range(1, n):
            pl.semaphore_signal(barrier, inc=1, **other(axis, lax.rem(at + d, n)))

    for slot in range(2):
        for k in range(levels, padded):
            n_buf[slot, k] = jnp.zeros((rows, lons), bf)
            u_buf[slot, k] = jnp.zeros((rows, lons), bf)
            c_buf[slot, k] = jnp.zeros((rows, lons), jnp.int32)
    for k in range(levels, padded):
        th_ref[k] = jnp.zeros((rows, lons), jnp.int32)
    b = b_ref[...]
    hb_ref[...] = jnp.where(b > 0, (b - 1) * 10, -100)
    z = jnp.zeros((128, lons), f32)
    m = jnp.concatenate([(b == v).astype(f32) for v in (1, 2, 3)]
                        + [jnp.zeros((128 - 3 * rows, lons), f32)], 0)
    m_row = lax.broadcasted_iota(jnp.int32, (128, lons), 0)
    for g in range(groups):
        mg = jnp.where(m_row % rows // 8 == g, m, 0.0)
        mk_ref[g] = jnp.concatenate(
            [jnp.concatenate([mg, z], 1), jnp.concatenate([z, mg], 1)], 0).astype(mk_ref.dtype)
    j = lax.broadcasted_iota(jnp.int32, (rows, lons), 0) + x * rows
    phi = (-78.0 + 156.0 * (j.astype(f32) + 0.5) / (rows * nlat)) * (math.pi / 180.0)
    zw = jnp.cos(phi)
    zn, zr = 0.02 * zw, 0.01 * zw

    i_row = lax.broadcasted_iota(jnp.int32, (8, 256), 0)
    i_col = lax.broadcasted_iota(jnp.int32, (8, 256), 1)

    def diagonal(v):
        v = [jnp.where(i_col % 8 == i_row, w, 0.0) for w in v]
        for n in (1, 2, 4):
            low = i_row & n == 0
            v = [jnp.where(low, p, q) + pltpu.roll(jnp.where(low, q, p), 8 - n, 0) for p, q in zip(v[::2], v[1::2])]
        return v[0]

    def to_owner(s):
        p = lax.rem(y + 1 + s, nlon)
        return [pltpu.make_async_remote_copy(
            src.at[s], dst.at[s], send_l.at[s, q], recv_l.at[s, q], **other("lon", p))
            for q, (src, dst) in enumerate(((t_ref, tb), (d_ref, db)))]

    def tables(accs, deps):
        @pl.loop(0, months)
        def _(s):
            slot = lax.rem(s, 2)
            @pl.when(s < months - 1)
            def _():
                for at in chunks:
                    for c in inputs(s + 1, *at):
                        c.start()

            @pl.loop(0, rounds)
            def _(r):
                for at in chunks:
                    @pl.when(r == at[0])
                    def _():
                        for c in inputs(s, *at):
                            c.wait()

                    @pl.when((r == at[0]) & (s == 0))
                    def _():
                        thick(*at).wait()

                @pl.when(s == 0)
                def _():
                    @pl.loop(0, chunk // 2)
                    def _(q):
                        for e in range(2):
                            k = r * chunk + 2 * q + e
                            th = th_ref[k]
                            cn_ref[k] = zn * (th.astype(f32) * 0.001)
                            cr_ref[k] = jnp.where(th > 0, zr, 0.0)

                for p in range(UNROLL):
                    for tile in range(groups // 2):
                        even, odd = (build(n_buf, u_buf, c_buf, cn_ref, cr_ref, hb_ref,
                                           slot, 2 * (r * UNROLL + p) + e, tile) for e in range(2))
                        for q in range(2):
                            g = 2 * tile + q
                            S, V, F = (jnp.concatenate([v, w], 1) for v, w in zip(even[q], odd[q]))
                            pltpu.matmul_push_rhs(S, staging_register=tile % 2, mxu_index=q, transpose=True)
                            pltpu.matmul_acc_lhs(accs[g], V, load_staged_rhs=tile % 2)
                            f_ref[g, r * UNROLL + p] = F

            for g in range(groups):
                for q in range(2):
                    pltpu.matmul_push_rhs(mk_ref[g], staging_register=g % 2, mxu_index=q, transpose=True)
                    pltpu.matmul_acc_lhs(
                        deps[q], f_ref[g, half * q:half * q + half].reshape(16 * half, 256), load_staged_rhs=g % 2)
            for g in range(groups):
                v = pltpu.matmul_pop(accs[g])
                for f in range(2):
                    t_ref[s, g, 8 * f:8 * f + 8, :] = diagonal(
                        [v[64 * f + 8 * l:64 * f + 8 * l + 8] for l in range(8)])
            for q in range(2):
                v = pltpu.matmul_pop(deps[q])
                for f in range(2):
                    for t in range(0, half, 8):
                        d_ref[s, f, q, t:t + 8, :] = diagonal(
                            [v[16 * p + 8 * f:16 * p + 8 * f + 8] if p < half else jnp.zeros((8, 256), f32)
                             for p in range(t, t + 8)])

            @pl.when(s == 0)
            def _():
                pl.semaphore_wait(barrier, nlon + nlat + nmem - 3)

            @pl.when(s < months - 1)
            def _():
                for c in to_owner(s):
                    c.start()

    pl.run_scoped(
        tables,
        tuple(pltpu.ACC(g % 2)((128, 256), f32) for g in range(groups)),
        tuple(pltpu.ACC(q)((16 * half, 256), f32) for q in range(2)))

    lane = lax.broadcasted_iota(jnp.int32, (8, 128), 1)
    wide = lax.broadcasted_iota(jnp.int32, (80, 128), 1)
    tall = lax.broadcasted_iota(jnp.int32, (80, 128), 0)

    def down(v):
        for s in (1, 2, 4, 8, 16, 32, 64):
            v = v + jnp.where(tall >= s, pltpu.roll(v, s, 0), 0.0)
        return v

    def along(v):
        s = 1
        while s < rows:
            v = v + jnp.where(wide % rows >= s, pltpu.roll(v, s, 1), 0.0)
            s *= 2
        return v

    def regions(v):
        w = pltpu.roll(v, rows, 1) + pltpu.roll(v, 2 * rows, 1) + pltpu.roll(v, 3 * rows, 1)
        return jnp.where((wide >= 3 * rows) & (wide < 4 * rows), w, v)

    sends_l = [c for s in range(months - 1) for c in to_owner(s)]
    for c in sends_l:
        c.wait_recv()

    def class_rows(f):
        R = {}
        for g in range(groups):
            T = t_ref[months - 1, g, 8 * f:8 * f + 8, :]
            for d in range(months - 1):
                T = T + tb[d, g, 8 * f:8 * f + 8, :]
            for q in range(3):
                s = (rows * q + 8 * g - 80 * q) % 256
                R[q, g] = pltpu.roll(T, s, 1) if s else T
        for h in range(10):
            z = jnp.zeros((8, 128), f32)
            for (q, g), v in R.items():
                o = groups * q + g + h
                z = jnp.where(lane // 8 == o % 16, v[:, :128] if o < 16 else v[:, 128:], z)
            a_ref[f, 8 * h:8 * h + 8, :] = pltpu.roll(z, 128 - 8 * h, 1) if h else z
        return regions(a_ref[f])

    def depth_rows(f):
        D = d_ref[months - 1, f]
        for d in range(months - 1):
            D = D + db[d, f]
        a_ref[2 + f, 72:80, :] = jnp.zeros((8, 128), f32)
        for q in range(2):
            for e in range(2):
                a_ref[2 + f, pl.ds(2 * half * q + e, half, stride=2), :] = D[q, :half, 128 * e:128 * e + 128]
        return regions(a_ref[2 + f])

    up = [down(along(class_rows(1))), along(depth_rows(1))]
    packed = jnp.zeros((8, 128), f32)
    for q in range(2):
        for v in range(10):
            r = (10 * q + v - (rows - 1)) % 128
            w = up[q][8 * v:8 * v + 8]
            packed = jnp.where(lane % rows == 10 * q + v, pltpu.roll(w, r, 1) if r else w, packed)
    pk[...] = packed
    sends_x = []
    for d in range(1, nlat):
        c = pltpu.make_async_remote_copy(
            pk, pb.at[d - 1], send_x.at[d - 1], recv_x.at[d - 1], **other("lat", lax.rem(x + d, nlat)))
        c.start()
        sends_x.append(c)

    core = lax.rem(me, 2)
    zz = (me - core) // 2
    far_first = sorted(range(1, nz), key=lambda d: (-min(d, nz - d), d))
    sends_m = []

    def piece_to(f, dz):
        to = 2 * lax.rem(zz + dz, nz) + f
        d = lax.rem(to - me + nmem, nmem)
        return pltpu.make_async_remote_copy(
            mine.at[to], got.at[d - 1], send_m.at[d - 1], recv_m.at[d - 1], **other("mem", to))

    def hand_in(f, tables_f):
        for q, v in enumerate(tables_f):
            a_ref[2 * q + f] = v
        for t in range(nz):
            mine[2 * t + f] = jnp.concatenate(
                [a_ref[2 * q + f, pl.ds(t, per, stride=nz), :] for q in range(2)], 0)
        for dz in far_first:
            c = piece_to(f, dz)
            c.start()
            sends_m.append(c)

        @pl.when(core != f)
        def _():
            piece_to(f, 0).start()

    hand_in(1, up)
    hand_in(0, [down(class_rows(0)), down(depth_rows(0))])

    carry = jnp.zeros((8, 128), f32)
    for d, c in enumerate(sends_x):
        c.wait_recv()
        carry = carry + jnp.where(x > d, pb[d], 0.0)
    for t in range(nz):
        cs[t] = carry[t:t + 1]

    def carry_to(dz):
        to = 2 * lax.rem(zz + dz, nz) + 1
        d = lax.rem(to - me + nmem, nmem)
        return pltpu.make_async_remote_copy(
            cs.at[lax.rem(zz + dz, nz)], cb.at[d - 1], send_c.at[d - 1], recv_c.at[d - 1], **other("mem", to))

    for dz in far_first:
        carry_to(dz).start()

    @pl.when(core == 0)
    def _():
        carry_to(0).start()

    p_row = lax.broadcasted_iota(jnp.int32, (piece, 128), 0)
    p_lane = lax.broadcasted_iota(jnp.int32, (piece, 128), 1)

    def spread_out(row):
        w = jnp.where(p_lane % rows == p_row, jnp.broadcast_to(row, (piece, 128)), 0.0)
        n = 1
        while n < rows:
            w = w + jnp.where(p_lane % rows >= n, pltpu.roll(w, n, 1), pltpu.roll(w, 128 - rows + n, 1))
            n *= 2
        return w

    for d in range(1, nmem):
        pltpu.make_async_remote_copy(
            mine.at[me], got.at[d - 1], send_m.at[d - 1], recv_m.at[d - 1],
            **other("mem", lax.rem(me + d, nmem))).wait_recv()
    all_m[0] = mine[me]
    for d in range(1, nmem):
        all_m[d] = got[d - 1]

    @pl.when(core == 1)
    def _():
        all_m[0] = all_m[0] + spread_out(cs[zz])
        for d in range(1, nmem):
            pltpu.make_async_remote_copy(
                cs.at[0], cb.at[d - 1], send_c.at[d - 1], recv_c.at[d - 1],
                **other("mem", lax.rem(me + d, nmem))).wait_recv()
        for d in range(1, nmem):
            all_m[d] = all_m[d] + spread_out(cb[d - 1])

    total = all_m[0]
    for d in range(1, nmem):
        total = total + all_m[d]
    mean = total * (1.0 / nmem)
    square = jnp.square(all_m[0] - mean)
    for d in range(1, nmem):
        square = square + jnp.square(all_m[d] - mean)
    res[me, 0] = mean
    res[me, 1] = jnp.sqrt(square * (1.0 / (nmem - 1)))

    partner = me + 1 - 2 * core
    sends_g = []

    def give(piece_of, to, slot):
        c = pltpu.make_async_remote_copy(
            res.at[piece_of], res.at[piece_of], send_g.at[slot], recv_g.at[piece_of], **other("mem", to))
        c.start()
        sends_g.append(c)

    def take(piece_of):
        pltpu.make_async_remote_copy(
            res.at[piece_of], res.at[piece_of], send_g.at[0], recv_g.at[piece_of], **other("mem", partner)).wait_recv()

    for dz in far_first:
        give(me, lax.rem(me + 2 * dz, nmem), 2 * dz)
    give(me, partner, 0)
    for dz in reversed(far_first):
        p = lax.rem(me + nmem - 2 * dz, nmem)
        take(p)
        give(p, partner, 2 * dz + 1)
    take(partner)
    for dz in reversed(far_first):
        take(lax.rem(partner + nmem - 2 * dz, nmem))

    all_ref[...] = res[...]
    for c in sends_l + sends_x + sends_g:
        c.wait_send()
    for dz in far_first:
        carry_to(dz).wait_send()

    @pl.when(core == 0)
    def _():
        carry_to(0).wait_send()

    for d in range(1, nmem):
        pltpu.make_async_remote_copy(
            mine.at[me], got.at[d - 1], send_m.at[d - 1], recv_m.at[d - 1],
            **other("mem", lax.rem(me + d, nmem))).wait_send()


def statistics(north, up, dens, thick, basin, nlon, nlat, nmem):
    f32, bf, i32 = jnp.float32, jnp.bfloat16, jnp.int32
    months, levels, rows, lons = north.shape
    groups = rows // 8
    npairs = UNROLL * -(-levels // (2 * UNROLL))
    padded = 2 * npairs
    piece = 320 // nmem
    vm = pl.BlockSpec(memory_space=pltpu.VMEM)
    hbm = pl.BlockSpec(memory_space=pl.ANY)
    sem = pltpu.SemaphoreType.DMA
    return pl.pallas_call(
        functools.partial(kernel, nlon, nlat, nmem),
        in_specs=[hbm, hbm, hbm, hbm, vm],
        out_specs=vm,
        out_shape=jax.ShapeDtypeStruct((nmem, 2, piece, 128), f32),
        scratch_shapes=[
            pltpu.VMEM((2, padded, rows, lons), bf),
            pltpu.VMEM((2, padded, rows, lons), bf),
            pltpu.VMEM((2, padded, rows, lons), i32),
            pltpu.VMEM((padded, rows, lons), i32),
            pltpu.VMEM((padded, rows, lons), f32),
            pltpu.VMEM((padded, rows, lons), f32),
            pltpu.VMEM((rows, lons), i32),
            pltpu.VMEM((groups, 256, 256), jnp.float8_e4m3fn),
            pltpu.VMEM((groups, npairs, 16, 256), bf),
            pltpu.VMEM((months, groups, 16, 256), f32),
            pltpu.VMEM((months, 2, 2, -(-(npairs // 2) // 8) * 8, 256), f32),
            pltpu.VMEM((months - 1, groups, 16, 256), f32),
            pltpu.VMEM((months - 1, 2, 2, -(-(npairs // 2) // 8) * 8, 256), f32),
            pltpu.VMEM((8, 128), f32),
            pltpu.VMEM((nlat - 1, 8, 128), f32),
            pltpu.VMEM((5, 80, 128), f32),
            pltpu.VMEM((nmem, piece, 128), f32),
            pltpu.VMEM((nmem - 1, piece, 128), f32),
            pltpu.VMEM((nmem, piece, 128), f32),
            pltpu.VMEM((nmem // 2, 1, 128), f32),
            pltpu.VMEM((nmem - 1, 1, 128), f32),
            pltpu.VMEM((nmem, 2, piece, 128), f32),
            sem((2, npairs // UNROLL, 3)), sem((npairs // UNROLL,)),
            sem((months - 1, 2)), sem((months - 1, 2)),
            sem((nlat - 1,)), sem((nlat - 1,)),
            sem((nmem - 1,)), sem((nmem - 1,)),
            sem((nmem - 1,)), sem((nmem - 1,)),
            sem((nmem,)), sem((nmem,)),
        ],
        compiler_params=pltpu.CompilerParams(
            collective_id=0, has_side_effects=True, vmem_limit_bytes=63 * 2**20),
        name="statistics",
    )(north, up, dens, thick, basin)


def finish_kernel(rows, all_ref, dm_ref, ds_ref, cm_ref, cs_ref, a_ref):
    nmem, piece = all_ref.shape[0], all_ref.shape[2]
    nz, per = nmem // 2, piece // 2
    a_ref[...] = jnp.zeros_like(a_ref)
    for k, outs in enumerate(((cm_ref, dm_ref), (cs_ref, ds_ref))):
        for a in range(4):
            for t in range(nz):
                v = all_ref[2 * t + a % 2, k]
                a_ref[4 * k + a, pl.ds(t, per, stride=nz), :] = v[per * (a // 2):per * (a // 2 + 1)]
        for a in range(4):
            v = a_ref[4 * k + a].T
            out = outs[a // 2]
            for r in range(4):
                s = rows * ((r + 3) % 4)
                out[0, r, a % 2] = v[s:s + rows, :out.shape[-1]]


def finish(res, levels, rows):
    f32 = jnp.float32
    vm = pl.BlockSpec(memory_space=pltpu.VMEM)
    dep = jax.ShapeDtypeStruct((1, 4, 2, rows, levels), f32)
    cla = jax.ShapeDtypeStruct((1, 4, 2, rows, 80), f32)
    outs = pl.pallas_call(
        functools.partial(finish_kernel, rows),
        in_specs=[vm],
        out_specs=[vm] * 4,
        out_shape=[dep, dep, cla, cla],
        scratch_shapes=[pltpu.VMEM((8, 128, 128), f32)],
        name="finish",
    )(res)
    return tuple(jnp.swapaxes(o, 3, 4) for o in outs)


def solution(mesh):
    nlon, nlat, nmem = (mesh.shape[a] for a in ("lon", "lat", "mem"))

    def body(north_vel, up_vel, dens_class, thickness, basin_id):
        res = statistics(north_vel[0], up_vel[0], dens_class[0], thickness, basin_id, nlon, nlat, nmem)
        return finish(res, *thickness.shape[:2])

    big = P("mem", None, None, "lat", "lon")
    out = P("lon", None, None, None, "lat")
    return jax.shard_map(
        body, mesh=mesh, in_specs=(big, big, big, P(None, "lat", "lon"), P("lat", "lon")),
        out_specs=(out,) * 4, check_vma=False)
```

```python
import functools
import math

import jax
import jax.numpy as jnp
from jax import lax
from jax.experimental import pallas as pl
from jax.experimental.pallas import tpu as pltpu
from jax.sharding import PartitionSpec as P

MESH = pl.DeviceIdType.MESH
UNROLL = 10


def build(n_ref, u_ref, c_ref, cn_ref, cr_ref, hb_ref, slot, k, tile):
    bf, f32, f8 = jnp.bfloat16, jnp.float32, jnp.float8_e4m3fn
    r0 = 16 * tile
    nf = n_ref[slot, k, r0:r0 + 16, :].astype(f32) * cn_ref[k, r0:r0 + 16, :]
    rf = u_ref[slot, k, r0:r0 + 16, :].astype(f32) * cr_ref[k, r0:r0 + 16, :]
    cc = c_ref[slot, k, r0:r0 + 16, :]
    hi = ((cc >> 3) + hb_ref[r0:r0 + 16, :]).astype(f32)
    lo = (cc & 7).astype(f32)
    zero = jnp.zeros((16, cc.shape[1]), bf)
    one = jnp.ones((16, cc.shape[1]), bf)
    out = []
    for s in range(2):
        a, b = nf[8 * s:8 * s + 8], rf[8 * s:8 * s + 8]
        h, l = hi[8 * s:8 * s + 8], lo[8 * s:8 * s + 8]
        nn = jnp.concatenate([a, a], 0).astype(bf)
        rr = jnp.concatenate([b, b], 0).astype(bf)
        fl = jnp.concatenate([a, b], 0).astype(bf)
        hh = jnp.concatenate([h, h - 1.0], 0).astype(bf)
        ll = jnp.concatenate([l, l - 1.0], 0).astype(bf)
        S = [jnp.where(hh == bf(2 * q), one, zero) for q in range(16)]
        S = [jnp.concatenate(S[2 * q:2 * q + 2], 0).astype(f8) for q in range(8)]
        ms = [ll == bf(2 * q) for q in range(4)]
        V = [jnp.where(m, nn, zero) for m in ms] + [jnp.where(m, rr, zero) for m in ms]
        out.append((jnp.concatenate(S, 0), jnp.concatenate(V, 0), fl))
    return out


def kernel(nlon, nlat, nmem, n_hbm, u_hbm, c_hbm, th_hbm, b_ref, all_ref,
           n_buf, u_buf, c_buf, th_ref, cn_ref, cr_ref, hb_ref, mk_ref, f_ref,
           t_ref, d_ref, tb, db, pk, pb, a_ref, mine, got, cs, cb, res,
           in_sem, th_sem, send_l, recv_l, send_x, recv_x, send_m, recv_m, send_c, recv_c, send_g, recv_g):
    bf, f32 = jnp.bfloat16, jnp.float32
    y, x, me = lax.axis_index("lon"), lax.axis_index("lat"), lax.axis_index("mem")
    months, levels, rows, lons = n_hbm.shape
    groups = rows // 8
    padded = cn_ref.shape[0]
    npairs = padded // 2
    half = npairs // 2
    rounds = npairs // UNROLL
    nz = nmem // 2
    per = 80 // nz
    piece = 2 * per

    def other(axis, index):
        return dict(device_id={axis: index}, device_id_type=MESH)

    chunk = 2 * UNROLL
    chunks = [(r, chunk * r, min(chunk, levels - chunk * r)) for r in range(rounds)]

    def inputs(s, r, k0, n):
        month, slot = lax.rem(y + 1 + s, months), lax.rem(s, 2)
        return [pltpu.make_async_copy(
            src.at[month, pl.ds(k0, n)], buf.at[slot, pl.ds(k0, n)], in_sem.at[slot, r, q])
            for q, (src, buf) in enumerate(((n_hbm, n_buf), (u_hbm, u_buf), (c_hbm, c_buf)))]

    def thick(r, k0, n):
        return pltpu.make_async_copy(th_hbm.at[pl.ds(k0, n)], th_ref.at[pl.ds(k0, n)], th_sem.at[r])

    for at in chunks:
        thick(*at).start()
        for c in inputs(0, *at):
            c.start()
    barrier = pltpu.get_barrier_semaphore()
    for axis, at, n in (("lon", y, nlon), ("lat", x, nlat), ("mem", me, nmem)):
        @pl.loop(1, n)
        def _(d):
            pl.semaphore_signal(barrier, inc=1, **other(axis, lax.rem(at + d, n)))


    for slot in range(2):
        for k in range(levels, padded):
            n_buf[slot, k] = jnp.zeros((rows, lons), bf)
            u_buf[slot, k] = jnp.zeros((rows, lons), bf)
            c_buf[slot, k] = jnp.zeros((rows, lons), jnp.int32)
    for k in range(levels, padded):
        th_ref[k] = jnp.zeros((rows, lons), jnp.int32)
    b = b_ref[...]
    hb_ref[...] = jnp.where(b > 0, (b - 1) * 10, -100)
    z = jnp.zeros((128, lons), f32)
    m = jnp.concatenate([(b == v).astype(f32) for v in (1, 2, 3)]
                        + [jnp.zeros((128 - 3 * rows, lons), f32)], 0)
    m_row = lax.broadcasted_iota(jnp.int32, (128, lons), 0)
    for g in range(groups):
        mg = jnp.where(m_row % rows // 8 == g, m, 0.0)
        mk_ref[g] = jnp.concatenate(
            [jnp.concatenate([mg, z], 1), jnp.concatenate([z, mg], 1)], 0).astype(mk_ref.dtype)
    j = lax.broadcasted_iota(jnp.int32, (rows, lons), 0) + x * rows
    phi = (-78.0 + 156.0 * (j.astype(f32) + 0.5) / (rows * nlat)) * (math.pi / 180.0)
    zw = jnp.cos(phi)
    zn, zr = 0.02 * zw, 0.01 * zw

    i_row = lax.broadcasted_iota(jnp.int32, (8, 256), 0)
    i_col = lax.broadcasted_iota(jnp.int32, (8, 256), 1)

    def diagonal(v):
        v = [jnp.where(i_col % 8 == i_row, w, 0.0) for w in v]
        for n in (1, 2, 4):
            low = i_row & n == 0
            v = [jnp.where(low, p, q) + pltpu.roll(jnp.where(low, q, p), 8 - n, 0) for p, q in zip(v[::2], v[1::2])]
        return v[0]

    def to_owner(s):
        p = lax.rem(y + 1 + s, nlon)
        return [pltpu.make_async_remote_copy(
            src.at[s], dst.at[s], send_l.at[s, q], recv_l.at[s, q], **other("lon", p))
            for q, (src, dst) in enumerate(((t_ref, tb), (d_ref, db)))]

    def tables(accs, deps):
        @pl.loop(0, months)
        def _(s):
            slot = lax.rem(s, 2)
            @pl.loop(0, rounds)
            def _(r):
                for at in chunks:
                    @pl.when(r == at[0])
                    def _():
                        for c in inputs(s, *at):
                            c.wait()

                    @pl.when((r == at[0]) & (s == 0))
                    def _():
                        thick(*at).wait()

                @pl.when((r == 1) & (s < months - 1))
                def _():
                    for at in chunks:
                        for c in inputs(s + 1, *at):
                            c.start()

                @pl.when(s == 0)
                def _():
                    @pl.loop(0, chunk // 2)
                    def _(q):
                        for e in range(2):
                            k = r * chunk + 2 * q + e
                            th = th_ref[k]
                            cn_ref[k] = zn * (th.astype(f32) * 0.001)
                            cr_ref[k] = jnp.where(th > 0, zr, 0.0)

                for p in range(UNROLL):
                    for tile in range(groups // 2):
                        even, odd = (build(n_buf, u_buf, c_buf, cn_ref, cr_ref, hb_ref,
                                           slot, 2 * (r * UNROLL + p) + e, tile) for e in range(2))
                        for q in range(2):
                            g = 2 * tile + q
                            S, V, F = (jnp.concatenate([v, w], 1) for v, w in zip(even[q], odd[q]))
                            pltpu.matmul_push_rhs(S, staging_register=tile % 2, mxu_index=q, transpose=True)
                            pltpu.matmul_acc_lhs(accs[g], V, load_staged_rhs=tile % 2)
                            f_ref[g, r * UNROLL + p] = F

            for g in range(groups):
                for q in range(2):
                    pltpu.matmul_push_rhs(mk_ref[g], staging_register=g % 2, mxu_index=q, transpose=True)
                    pltpu.matmul_acc_lhs(
                        deps[q], f_ref[g, half * q:half * q + half].reshape(16 * half, 256), load_staged_rhs=g % 2)
            for g in range(groups):
                v = pltpu.matmul_pop(accs[g])
                for f in range(2):
                    t_ref[s, g, 8 * f:8 * f + 8, :] = diagonal(
                        [v[64 * f + 8 * l:64 * f + 8 * l + 8] for l in range(8)])
            for q in range(2):
                v = pltpu.matmul_pop(deps[q])
                for f in range(2):
                    for t in range(0, half, 8):
                        d_ref[s, f, q, t:t + 8, :] = diagonal(
                            [v[16 * p + 8 * f:16 * p + 8 * f + 8] if p < half else jnp.zeros((8, 256), f32)
                             for p in range(t, t + 8)])

            @pl.when(s == 0)
            def _():
                pl.semaphore_wait(barrier, nlon + nlat + nmem - 3)

            @pl.when(s < months - 1)
            def _():
                for c in to_owner(s):
                    c.start()

    pl.run_scoped(
        tables,
        tuple(pltpu.ACC(g % 2)((128, 256), f32) for g in range(groups)),
        tuple(pltpu.ACC(q)((16 * half, 256), f32) for q in range(2)))

    lane = lax.broadcasted_iota(jnp.int32, (8, 128), 1)
    wide = lax.broadcasted_iota(jnp.int32, (80, 128), 1)
    tall = lax.broadcasted_iota(jnp.int32, (80, 128), 0)

    def down(v):
        for s in (1, 2, 4, 8, 16, 32, 64):
            v = v + jnp.where(tall >= s, pltpu.roll(v, s, 0), 0.0)
        return v

    def along(v):
        s = 1
        while s < rows:
            v = v + jnp.where(wide % rows >= s, pltpu.roll(v, s, 1), 0.0)
            s *= 2
        return v

    def regions(v):
        w = pltpu.roll(v, rows, 1) + pltpu.roll(v, 2 * rows, 1) + pltpu.roll(v, 3 * rows, 1)
        return jnp.where((wide >= 3 * rows) & (wide < 4 * rows), w, v)

    sends_l = [c for s in range(months - 1) for c in to_owner(s)]
    for c in sends_l:
        c.wait_recv()

    def class_rows(f):
        R = {}
        for g in range(groups):
            T = t_ref[months - 1, g, 8 * f:8 * f + 8, :]
            for d in range(months - 1):
                T = T + tb[d, g, 8 * f:8 * f + 8, :]
            for q in range(3):
                s = (rows * q + 8 * g - 80 * q) % 256
                R[q, g] = pltpu.roll(T, s, 1) if s else T
        for h in range(10):
            z = jnp.zeros((8, 128), f32)
            for (q, g), v in R.items():
                o = groups * q + g + h
                z = jnp.where(lane // 8 == o % 16, v[:, :128] if o < 16 else v[:, 128:], z)
            a_ref[f, 8 * h:8 * h + 8, :] = pltpu.roll(z, 128 - 8 * h, 1) if h else z
        return regions(a_ref[f])

    def depth_rows(f):
        D = d_ref[months - 1, f]
        for d in range(months - 1):
            D = D + db[d, f]
        a_ref[2 + f, 72:80, :] = jnp.zeros((8, 128), f32)
        for q in range(2):
            for e in range(2):
                a_ref[2 + f, pl.ds(2 * half * q + e, half, stride=2), :] = D[q, :half, 128 * e:128 * e + 128]
        return regions(a_ref[2 + f])

    up = [down(along(class_rows(1))), along(depth_rows(1))]
    packed = jnp.zeros((8, 128), f32)
    for q in range(2):
        for v in range(10):
            r = (10 * q + v - (rows - 1)) % 128
            w = up[q][8 * v:8 * v + 8]
            packed = jnp.where(lane % rows == 10 * q + v, pltpu.roll(w, r, 1) if r else w, packed)
    pk[...] = packed
    sends_x = []
    for d in range(1, nlat):
        c = pltpu.make_async_remote_copy(
            pk, pb.at[d - 1], send_x.at[d - 1], recv_x.at[d - 1], **other("lat", lax.rem(x + d, nlat)))
        c.start()
        sends_x.append(c)

    core = lax.rem(me, 2)
    zz = (me - core) // 2

    def far_first(k):
        return nz // 2 + (k + 1) // 2 * (1 - 2 * lax.rem(k, 2))

    def piece_to(f, dz):
        to = 2 * lax.rem(zz + dz, nz) + f
        d = lax.rem(to - me + nmem, nmem)
        return pltpu.make_async_remote_copy(
            mine.at[to], got.at[d], send_m.at[d - 1], recv_m.at[d - 1], **other("mem", to))

    def hand_in(f, tables_f):
        for q, v in enumerate(tables_f):
            a_ref[2 * q + f] = v
        for t in range(nz):
            mine[2 * t + f] = jnp.concatenate(
                [a_ref[2 * q + f, pl.ds(t, per, stride=nz), :] for q in range(2)], 0)
        @pl.loop(0, nz - 1)
        def _(k):
            piece_to(f, far_first(k)).start()

        @pl.when(core != f)
        def _():
            piece_to(f, 0).start()

    hand_in(1, up)
    hand_in(0, [down(class_rows(0)), down(depth_rows(0))])

    carry = jnp.zeros((8, 128), f32)
    for d, c in enumerate(sends_x):
        c.wait_recv()
        carry = carry + jnp.where(x > d, pb[d], 0.0)
    for t in range(nz):
        cs[t] = carry[t:t + 1]

    def carry_to(dz):
        to = 2 * lax.rem(zz + dz, nz) + 1
        d = lax.rem(to - me + nmem, nmem)
        return pltpu.make_async_remote_copy(
            cs.at[lax.rem(zz + dz, nz)], cb.at[d - 1], send_c.at[d - 1], recv_c.at[d - 1], **other("mem", to))

    @pl.loop(1, nz)
    def _(dz):
        carry_to(dz).start()

    @pl.when(core == 0)
    def _():
        carry_to(0).start()

    p_row = lax.broadcasted_iota(jnp.int32, (piece, 128), 0)
    p_lane = lax.broadcasted_iota(jnp.int32, (piece, 128), 1)

    def spread_out(row):
        w = jnp.where(p_lane % rows == p_row, jnp.broadcast_to(row, (piece, 128)), 0.0)
        n = 1
        while n < rows:
            w = w + jnp.where(p_lane % rows >= n, pltpu.roll(w, n, 1), pltpu.roll(w, 128 - rows + n, 1))
            n *= 2
        return w

    def piece_from(d):
        return pltpu.make_async_remote_copy(
            mine.at[me], got.at[d], send_m.at[d - 1], recv_m.at[d - 1], **other("mem", lax.rem(me + d, nmem)))

    def carry_from(d):
        return pltpu.make_async_remote_copy(
            cs.at[0], cb.at[d - 1], send_c.at[d - 1], recv_c.at[d - 1], **other("mem", lax.rem(me + d, nmem)))

    got[0] = mine[me]

    @pl.loop(1, nmem)
    def _(d):
        piece_from(d).wait_recv()

    @pl.when(core == 1)
    def _():
        got[0] = got[0] + spread_out(cs[zz])

        @pl.loop(1, nmem)
        def _(d):
            carry_from(d).wait_recv()

        @pl.loop(0, (nmem - 1) // 3)
        def _(q):
            for e in range(3):
                d = 3 * q + e + 1
                got[d] = got[d] + spread_out(cb[d - 1])

    total = got[0]
    for d in range(1, nmem):
        total = total + got[d]
    mean = total * (1.0 / nmem)
    square = jnp.square(got[0] - mean)
    for d in range(1, nmem):
        square = square + jnp.square(got[d] - mean)
    res[me, 0] = mean
    res[me, 1] = jnp.sqrt(square * (1.0 / (nmem - 1)))

    partner = me + 1 - 2 * core

    def give(piece_of, to, slot):
        return pltpu.make_async_remote_copy(
            res.at[piece_of], res.at[piece_of], send_g.at[slot], recv_g.at[piece_of], **other("mem", to))

    def give_far(dz):
        return give(me, lax.rem(me + 2 * dz, nmem), 2 * dz)

    def pass_on(dz):
        return give(lax.rem(me + nmem - 2 * dz, nmem), partner, 2 * dz + 1)

    @pl.loop(0, nz - 1)
    def _(k):
        give_far(far_first(k)).start()

    give(me, partner, 0).start()

    @pl.loop(1, nmem)
    def _(d):
        piece_from(d).wait_send()

    @pl.loop(1, nz)
    def _(dz):
        carry_to(dz).wait_send()

    @pl.when(core == 0)
    def _():
        carry_to(0).wait_send()

    for c in sends_l + sends_x:
        c.wait_send()

    @pl.loop(0, nz - 1)
    def _(k):
        dz = far_first(nz - 2 - k)
        give(lax.rem(me + nmem - 2 * dz, nmem), partner, 0).wait_recv()
        pass_on(dz).start()

    @pl.loop(0, nz)
    def _(k):
        give(lax.rem(partner + 2 * k, nmem), partner, 0).wait_recv()

    all_ref[...] = res[...]
    @pl.loop(1, nz)
    def _(dz):
        give_far(dz).wait_send()
        pass_on(dz).wait_send()

    give(me, partner, 0).wait_send()


def statistics(north, up, dens, thick, basin, nlon, nlat, nmem):
    f32, bf, i32 = jnp.float32, jnp.bfloat16, jnp.int32
    months, levels, rows, lons = north.shape
    groups = rows // 8
    npairs = UNROLL * -(-levels // (2 * UNROLL))
    padded = 2 * npairs
    piece = 320 // nmem
    vm = pl.BlockSpec(memory_space=pltpu.VMEM)
    hbm = pl.BlockSpec(memory_space=pl.ANY)
    sem = pltpu.SemaphoreType.DMA
    return pl.pallas_call(
        functools.partial(kernel, nlon, nlat, nmem),
        in_specs=[hbm, hbm, hbm, hbm, vm],
        out_specs=vm,
        out_shape=jax.ShapeDtypeStruct((nmem, 2, piece, 128), f32),
        scratch_shapes=[
            pltpu.VMEM((2, padded, rows, lons), bf),
            pltpu.VMEM((2, padded, rows, lons), bf),
            pltpu.VMEM((2, padded, rows, lons), i32),
            pltpu.VMEM((padded, rows, lons), i32),
            pltpu.VMEM((padded, rows, lons), f32),
            pltpu.VMEM((padded, rows, lons), f32),
            pltpu.VMEM((rows, lons), i32),
            pltpu.VMEM((groups, 256, 256), jnp.float8_e4m3fn),
            pltpu.VMEM((groups, npairs, 16, 256), bf),
            pltpu.VMEM((months, groups, 16, 256), f32),
            pltpu.VMEM((months, 2, 2, -(-(npairs // 2) // 8) * 8, 256), f32),
            pltpu.VMEM((months - 1, groups, 16, 256), f32),
            pltpu.VMEM((months - 1, 2, 2, -(-(npairs // 2) // 8) * 8, 256), f32),
            pltpu.VMEM((8, 128), f32),
            pltpu.VMEM((nlat - 1, 8, 128), f32),
            pltpu.VMEM((5, 80, 128), f32),
            pltpu.VMEM((nmem, piece, 128), f32),
            pltpu.VMEM((nmem, piece, 128), f32),
            pltpu.VMEM((nmem // 2, 1, 128), f32),
            pltpu.VMEM((nmem - 1, 1, 128), f32),
            pltpu.VMEM((nmem, 2, piece, 128), f32),
            sem((2, npairs // UNROLL, 3)), sem((npairs // UNROLL,)),
            sem((months - 1, 2)), sem((months - 1, 2)),
            sem((nlat - 1,)), sem((nlat - 1,)),
            sem((nmem - 1,)), sem((nmem - 1,)),
            sem((nmem - 1,)), sem((nmem - 1,)),
            sem((nmem,)), sem((nmem,)),
        ],
        compiler_params=pltpu.CompilerParams(
            collective_id=0, has_side_effects=True, vmem_limit_bytes=63 * 2**20),
        name="statistics",
    )(north, up, dens, thick, basin)


def finish_kernel(rows, all_ref, dm_ref, ds_ref, cm_ref, cs_ref, a_ref):
    nmem, piece = all_ref.shape[0], all_ref.shape[2]
    nz, per = nmem // 2, piece // 2
    a_ref[...] = jnp.zeros_like(a_ref)
    for k, outs in enumerate(((cm_ref, dm_ref), (cs_ref, ds_ref))):
        for a in range(4):
            for t in range(nz):
                v = all_ref[2 * t + a % 2, k]
                a_ref[4 * k + a, pl.ds(t, per, stride=nz), :] = v[per * (a // 2):per * (a // 2 + 1)]
        for a in range(4):
            v = a_ref[4 * k + a].T
            out = outs[a // 2]
            for r in range(4):
                s = rows * ((r + 3) % 4)
                out[0, r, a % 2] = v[s:s + rows, :out.shape[-1]]


def finish(res, levels, rows):
    f32 = jnp.float32
    vm = pl.BlockSpec(memory_space=pltpu.VMEM)
    dep = jax.ShapeDtypeStruct((1, 4, 2, rows, levels), f32)
    cla = jax.ShapeDtypeStruct((1, 4, 2, rows, 80), f32)
    outs = pl.pallas_call(
        functools.partial(finish_kernel, rows),
        in_specs=[vm],
        out_specs=[vm] * 4,
        out_shape=[dep, dep, cla, cla],
        scratch_shapes=[pltpu.VMEM((8, 128, 128), f32)],
        name="finish",
    )(res)
    return tuple(jnp.swapaxes(o, 3, 4) for o in outs)


def solution(mesh):
    nlon, nlat, nmem = (mesh.shape[a] for a in ("lon", "lat", "mem"))

    def body(north_vel, up_vel, dens_class, thickness, basin_id):
        res = statistics(north_vel[0], up_vel[0], dens_class[0], thickness, basin_id, nlon, nlat, nmem)
        return finish(res, *thickness.shape[:2])

    big = P("mem", None, None, "lat", "lon")
    out = P("lon", None, None, None, "lat")
    return jax.shard_map(
        body, mesh=mesh, in_specs=(big, big, big, P(None, "lat", "lon"), P("lat", "lon")),
        out_specs=(out,) * 4, check_vma=False)
```

```python
import functools
import math

import jax
import jax.numpy as jnp
from jax import lax
from jax.experimental import pallas as pl
from jax.experimental.pallas import tpu as pltpu
from jax.sharding import PartitionSpec as P

MESH = pl.DeviceIdType.MESH
PIECE = 320
UNROLL = 19


def build(n_ref, u_ref, c_ref, cn_ref, cr_ref, hb_ref, slot, k, tile):
    bf, f32, f8 = jnp.bfloat16, jnp.float32, jnp.float8_e4m3fn
    r0 = 16 * tile
    nf = n_ref[slot, k, r0:r0 + 16, :].astype(f32) * cn_ref[k, r0:r0 + 16, :]
    rf = u_ref[slot, k, r0:r0 + 16, :].astype(f32) * cr_ref[k, r0:r0 + 16, :]
    cc = c_ref[slot, k, r0:r0 + 16, :]
    hi = ((cc >> 3) + hb_ref[r0:r0 + 16, :]).astype(f32)
    lo = (cc & 7).astype(f32)
    zero = jnp.zeros((16, cc.shape[1]), bf)
    one = jnp.ones((16, cc.shape[1]), bf)
    out = []
    for s in range(2):
        a, b = nf[8 * s:8 * s + 8], rf[8 * s:8 * s + 8]
        h, l = hi[8 * s:8 * s + 8], lo[8 * s:8 * s + 8]
        nn = jnp.concatenate([a, a], 0).astype(bf)
        rr = jnp.concatenate([b, b], 0).astype(bf)
        fl = jnp.concatenate([a, b], 0).astype(bf)
        hh = jnp.concatenate([h, h - 1.0], 0).astype(bf)
        ll = jnp.concatenate([l, l - 1.0], 0).astype(bf)
        S = [jnp.where(hh == bf(2 * q), one, zero) for q in range(16)]
        S = [jnp.concatenate(S[2 * q:2 * q + 2], 0).astype(f8) for q in range(8)]
        ms = [ll == bf(2 * q) for q in range(4)]
        V = [jnp.where(m, nn, zero) for m in ms] + [jnp.where(m, rr, zero) for m in ms]
        out.append((jnp.concatenate(S, 0), jnp.concatenate(V, 0), fl))
    return out


def kernel(nlon, nlat, nmem, n_hbm, u_hbm, c_hbm, th_hbm, b_ref, all_ref,
           n_buf, u_buf, c_buf, th_ref, cn_ref, cr_ref, hb_ref, mk_ref, f_ref,
           t_ref, d_ref, tb, db, pk, pb, a_ref, mine, got, res,
           in_sem, th_sem, send_l, recv_l, send_x, recv_x, send_m, recv_m, send_g, recv_g):
    bf, f32 = jnp.bfloat16, jnp.float32
    y, x, me = lax.axis_index("lon"), lax.axis_index("lat"), lax.axis_index("mem")
    months, levels, rows, lons = n_hbm.shape
    groups = rows // 8
    padded = cn_ref.shape[0]
    npairs = padded // 2
    half = npairs // 2
    rounds = npairs // UNROLL
    nz = nmem // 2
    piece = PIECE // nmem

    def other(axis, index):
        return dict(device_id={axis: index}, device_id_type=MESH)

    def inputs(s):
        month, slot = lax.rem(y + 1 + s, months), lax.rem(s, 2)
        return [pltpu.make_async_copy(src.at[month], buf.at[slot, pl.ds(0, levels)], in_sem.at[slot, q])
                for q, (src, buf) in enumerate(((n_hbm, n_buf), (u_hbm, u_buf), (c_hbm, c_buf)))]

    th_copy = pltpu.make_async_copy(th_hbm, th_ref, th_sem)
    th_copy.start()
    for c in inputs(0):
        c.start()

    barrier = pltpu.get_barrier_semaphore()
    for axis, at, n in (("lon", y, nlon), ("lat", x, nlat), ("mem", me, nmem)):
        for d in range(1, n):
            pl.semaphore_signal(barrier, inc=1, **other(axis, lax.rem(at + d, n)))

    for slot in range(2):
        for k in range(levels, padded):
            n_buf[slot, k] = jnp.zeros((rows, lons), bf)
            u_buf[slot, k] = jnp.zeros((rows, lons), bf)
            c_buf[slot, k] = jnp.zeros((rows, lons), jnp.int32)
    for k in range(levels, padded):
        cn_ref[k] = jnp.zeros((rows, lons), f32)
        cr_ref[k] = jnp.zeros((rows, lons), f32)
    b = b_ref[...]
    hb_ref[...] = jnp.where(b > 0, (b - 1) * 10, -100)
    z = jnp.zeros((128, lons), bf)
    m = jnp.concatenate([(b == v).astype(f32) for v in (1, 2, 3)]
                        + [jnp.zeros((128 - 3 * rows, lons), f32)], 0).astype(bf)
    mk_ref[...] = jnp.concatenate([jnp.concatenate([m, z], 1), jnp.concatenate([z, m], 1)], 0)
    j = lax.broadcasted_iota(jnp.int32, (rows, lons), 0) + x * rows
    phi = (-78.0 + 156.0 * (j.astype(f32) + 0.5) / (rows * nlat)) * (math.pi / 180.0)
    zw = jnp.cos(phi)
    zn, zr = 0.02 * zw, 0.01 * zw
    th_copy.wait()

    @pl.loop(0, levels // 5)
    def _(q):
        for k in range(5):
            th = th_ref[5 * q + k]
            cn_ref[5 * q + k] = zn * (th.astype(f32) * 0.001)
            cr_ref[5 * q + k] = jnp.where(th > 0, zr, 0.0)

    for k in range(levels // 5 * 5, levels):
        th = th_ref[k]
        cn_ref[k] = zn * (th.astype(f32) * 0.001)
        cr_ref[k] = jnp.where(th > 0, zr, 0.0)

    i_row = lax.broadcasted_iota(jnp.int32, (8, 256), 0)
    i_col = lax.broadcasted_iota(jnp.int32, (8, 256), 1)

    def diagonal(v):
        v = [jnp.where(i_col % 8 == i_row, w, 0.0) for w in v]
        for n in (1, 2, 4):
            low = i_row & n == 0
            v = [jnp.where(low, p, q) + pltpu.roll(jnp.where(low, q, p), 8 - n, 0) for p, q in zip(v[::2], v[1::2])]
        return v[0]

    def to_owner(s):
        p = lax.rem(y + 1 + s, nlon)
        return [pltpu.make_async_remote_copy(
            src.at[s], dst.at[s], send_l.at[s, q], recv_l.at[s, q], **other("lon", p))
            for q, (src, dst) in enumerate(((t_ref, tb), (d_ref, db)))]

    def tables(accs, deps):
        @pl.loop(0, months)
        def _(s):
            slot = lax.rem(s, 2)
            for c in inputs(s):
                c.wait()

            @pl.when(s < months - 1)
            def _():
                for c in inputs(s + 1):
                    c.start()

            @pl.loop(0, rounds)
            def _(r):
                for p in range(UNROLL):
                    for tile in range(groups // 2):
                        even, odd = (build(n_buf, u_buf, c_buf, cn_ref, cr_ref, hb_ref,
                                           slot, 2 * (r * UNROLL + p) + e, tile) for e in range(2))
                        for q in range(2):
                            g = 2 * tile + q
                            S, V, F = (jnp.concatenate([v, w], 1) for v, w in zip(even[q], odd[q]))
                            pltpu.matmul_push_rhs(S, staging_register=tile % 2, mxu_index=q, transpose=True)
                            pltpu.matmul_acc_lhs(accs[g], V, load_staged_rhs=tile % 2)
                            f_ref[g, r * UNROLL + p] = F

            for q in range(2):
                pltpu.matmul_push_rhs(mk_ref[...], staging_register=0, mxu_index=q, transpose=True)
            for g in range(groups):
                v = pltpu.matmul_pop(accs[g])
                for f in range(2):
                    t_ref[s, g, 8 * f:8 * f + 8, :] = diagonal(
                        [v[64 * f + 8 * l:64 * f + 8 * l + 8] for l in range(8)])
            for h in range(2):
                tot = [0.0, 0.0]
                for g in range(groups):
                    pltpu.matmul_acc_lhs(
                        deps[g], f_ref[g, half * h:half * h + half].reshape(16 * half, 256),
                        load_staged_rhs=0 if g < 2 and h == 0 else None)
                for g in range(groups):
                    R = pltpu.matmul_pop(deps[g]).reshape(half, 2, 8, 256)
                    for f in range(2):
                        tot[f] = tot[f] + jnp.where((i_col % rows) == i_row + 8 * g, R[:, f], 0.0)
                for f in range(2):
                    d_ref[s, f, half * h:half * h + half, :] = jnp.sum(tot[f], axis=1)

            @pl.when(s == 0)
            def _():
                pl.semaphore_wait(barrier, nlon + nlat + nmem - 3)

            @pl.when(s < months - 1)
            def _():
                for c in to_owner(s):
                    c.start()

    pl.run_scoped(
        tables,
        tuple(pltpu.ACC(g % 2)((128, 256), f32) for g in range(groups)),
        tuple(pltpu.ACC(g % 2)((16 * half, 256), f32) for g in range(groups)))

    lane = lax.broadcasted_iota(jnp.int32, (8, 128), 1)
    wide = lax.broadcasted_iota(jnp.int32, (80, 128), 1)
    tall = lax.broadcasted_iota(jnp.int32, (80, 128), 0)

    def down(v):
        for s in (1, 2, 4, 8, 16, 32, 64):
            v = v + jnp.where(tall >= s, pltpu.roll(v, s, 0), 0.0)
        return v

    def along(v):
        s = 1
        while s < rows:
            v = v + jnp.where(wide % rows >= s, pltpu.roll(v, s, 1), 0.0)
            s *= 2
        return v

    def regions(v):
        w = pltpu.roll(v, rows, 1) + pltpu.roll(v, 2 * rows, 1) + pltpu.roll(v, 3 * rows, 1)
        return jnp.where((wide >= 3 * rows) & (wide < 4 * rows), w, v)

    sends_l = [c for s in range(months - 1) for c in to_owner(s)]
    for c in sends_l:
        c.wait_recv()

    def class_rows(f):
        R = {}
        for g in range(groups):
            T = t_ref[months - 1, g, 8 * f:8 * f + 8, :]
            for d in range(months - 1):
                T = T + tb[d, g, 8 * f:8 * f + 8, :]
            for q in range(3):
                s = (rows * q + 8 * g - 80 * q) % 256
                R[q, g] = pltpu.roll(T, s, 1) if s else T
        for h in range(10):
            z = jnp.zeros((8, 128), f32)
            for (q, g), v in R.items():
                o = groups * q + g + h
                z = jnp.where(lane // 8 == o % 16, v[:, :128] if o < 16 else v[:, 128:], z)
            a_ref[f, 8 * h:8 * h + 8, :] = pltpu.roll(z, 128 - 8 * h, 1) if h else z
        return regions(a_ref[f])

    def depth_rows(f):
        D = d_ref[months - 1, f]
        for d in range(months - 1):
            D = D + db[d, f]
        a_ref[2 + f, 72:80, :] = jnp.zeros((8, 128), f32)
        a_ref[2 + f, pl.ds(0, npairs, stride=2), :] = D[:, 0:128]
        a_ref[2 + f, pl.ds(1, npairs, stride=2), :] = D[:, 128:256]
        return regions(a_ref[2 + f])

    up = [along(class_rows(1)), along(depth_rows(1))]
    packed = jnp.zeros((8, 128), f32)
    for q in range(2):
        for v in range(10):
            r = (10 * q + v - (rows - 1)) % 128
            w = up[q][8 * v:8 * v + 8]
            packed = jnp.where(lane % rows == 10 * q + v, pltpu.roll(w, r, 1) if r else w, packed)
    pk[...] = packed
    sends_x = []
    for d in range(1, nlat):
        c = pltpu.make_async_remote_copy(
            pk, pb.at[d - 1], send_x.at[d - 1], recv_x.at[d - 1], **other("lat", lax.rem(x + d, nlat)))
        c.start()
        sends_x.append(c)

    core = lax.rem(me, 2)
    zz = (me - core) // 2
    far_first = sorted(range(1, nz), key=lambda d: (-min(d, nz - d), d))
    sends_m = []

    def piece_to(f, dz):
        to = 2 * lax.rem(zz + dz, nz) + f
        d = lax.rem(to - me + nmem, nmem)
        return pltpu.make_async_remote_copy(
            mine.at[to], got.at[d - 1], send_m.at[d - 1], recv_m.at[d - 1], **other("mem", to))

    def hand_in(f, tables_f):
        for q, v in enumerate(tables_f):
            a_ref[2 * q + f] = v
            for t in range(nz // 2):
                mine[2 * (q * (nz // 2) + t) + f] = a_ref[2 * q + f, piece * t:piece * t + piece, :]
        for dz in far_first:
            c = piece_to(f, dz)
            c.start()
            sends_m.append(c)

        @pl.when(core != f)
        def _():
            piece_to(f, 0).start()

    hand_in(0, [down(class_rows(0)), down(depth_rows(0))])

    carry = jnp.zeros((8, 128), f32)
    for d, c in enumerate(sends_x):
        c.wait_recv()
        carry = carry + jnp.where(x > d, pb[d], 0.0)
    for q in range(2):
        parts = []
        for v in range(10):
            r = (-(10 * q + v)) % 128
            w = pltpu.roll(carry, r, 1) if r else carry
            parts.append(jnp.where((lane % rows == 0) & (lane < 4 * rows), w, 0.0))
        up[q] = up[q] + along(jnp.concatenate(parts, 0))
    hand_in(1, [down(up[0]), up[1]])

    own = mine[me]
    total = own
    for d in range(1, nmem):
        pltpu.make_async_remote_copy(
            mine.at[me], got.at[d - 1], send_m.at[d - 1], recv_m.at[d - 1],
            **other("mem", lax.rem(me + d, nmem))).wait_recv()
        total = total + got[d - 1]
    mean = total * (1.0 / nmem)
    square = jnp.square(own - mean)
    for d in range(nmem - 1):
        square = square + jnp.square(got[d] - mean)
    res[me, 0] = mean
    res[me, 1] = jnp.sqrt(square * (1.0 / (nmem - 1)))

    partner = me + 1 - 2 * core
    sends_g = []

    def give(piece_of, to, slot):
        c = pltpu.make_async_remote_copy(
            res.at[piece_of], res.at[piece_of], send_g.at[slot], recv_g.at[piece_of], **other("mem", to))
        c.start()
        sends_g.append(c)

    def take(piece_of):
        pltpu.make_async_remote_copy(
            res.at[piece_of], res.at[piece_of], send_g.at[0], recv_g.at[piece_of], **other("mem", partner)).wait_recv()

    for dz in far_first:
        give(me, lax.rem(me + 2 * dz, nmem), 2 * dz)
    give(me, partner, 0)
    for c in sends_l + sends_x:
        c.wait_send()
    for d in range(1, nmem):
        pltpu.make_async_remote_copy(
            mine.at[me], got.at[d - 1], send_m.at[d - 1], recv_m.at[d - 1],
            **other("mem", lax.rem(me + d, nmem))).wait_send()
    for dz in reversed(far_first):
        p = lax.rem(me + nmem - 2 * dz, nmem)
        take(p)
        give(p, partner, 2 * dz + 1)
    take(partner)
    for dz in reversed(far_first):
        take(lax.rem(partner + nmem - 2 * dz, nmem))

    all_ref[...] = res[...]
    for c in sends_g:
        c.wait_send()


def statistics(north, up, dens, thick, basin, nlon, nlat, nmem):
    f32, bf, i32 = jnp.float32, jnp.bfloat16, jnp.int32
    months, levels, rows, lons = north.shape
    groups = rows // 8
    npairs = UNROLL * -(-levels // (2 * UNROLL))
    padded = 2 * npairs
    piece = PIECE // nmem
    vm = pl.BlockSpec(memory_space=pltpu.VMEM)
    hbm = pl.BlockSpec(memory_space=pl.ANY)
    sem = pltpu.SemaphoreType.DMA
    return pl.pallas_call(
        functools.partial(kernel, nlon, nlat, nmem),
        in_specs=[hbm, hbm, hbm, hbm, vm],
        out_specs=vm,
        out_shape=jax.ShapeDtypeStruct((nmem, 2, piece, 128), f32),
        scratch_shapes=[
            pltpu.VMEM((2, padded, rows, lons), bf),
            pltpu.VMEM((2, padded, rows, lons), bf),
            pltpu.VMEM((2, padded, rows, lons), i32),
            pltpu.VMEM((levels, rows, lons), i32),
            pltpu.VMEM((padded, rows, lons), f32),
            pltpu.VMEM((padded, rows, lons), f32),
            pltpu.VMEM((rows, lons), i32),
            pltpu.VMEM((256, 256), bf),
            pltpu.VMEM((groups, npairs, 16, 256), bf),
            pltpu.VMEM((months, groups, 16, 256), f32),
            pltpu.VMEM((months, 2, npairs, 256), f32),
            pltpu.VMEM((months - 1, groups, 16, 256), f32),
            pltpu.VMEM((months - 1, 2, npairs, 256), f32),
            pltpu.VMEM((8, 128), f32),
            pltpu.VMEM((nlat - 1, 8, 128), f32),
            pltpu.VMEM((5, 80, 128), f32),
            pltpu.VMEM((nmem, piece, 128), f32),
            pltpu.VMEM((nmem - 1, piece, 128), f32),
            pltpu.VMEM((nmem, 2, piece, 128), f32),
            sem((2, 3)), sem,
            sem((months - 1, 2)), sem((months - 1, 2)),
            sem((nlat - 1,)), sem((nlat - 1,)),
            sem((nmem - 1,)), sem((nmem - 1,)),
            sem((nmem,)), sem((nmem,)),
        ],
        compiler_params=pltpu.CompilerParams(
            collective_id=0, has_side_effects=True, vmem_limit_bytes=63 * 2**20),
        name="statistics",
    )(north, up, dens, thick, basin)


def finish_kernel(rows, all_ref, dm_ref, ds_ref, cm_ref, cs_ref, a_ref):
    nmem, piece = all_ref.shape[0], all_ref.shape[2]
    share = nmem // 4
    a_ref[...] = jnp.zeros_like(a_ref)
    for k, outs in enumerate(((cm_ref, dm_ref), (cs_ref, ds_ref))):
        for a in range(4):
            for t in range(share):
                o = 2 * (a // 2 * share + t) + a % 2
                a_ref[4 * k + a, piece * t:piece * t + piece, :] = all_ref[o, k]
        for a in range(4):
            v = a_ref[4 * k + a].T
            out = outs[a // 2]
            for r in range(4):
                s = rows * ((r + 3) % 4)
                out[0, r, a % 2] = v[s:s + rows, :out.shape[-1]]


def finish(res, levels, rows):
    f32 = jnp.float32
    vm = pl.BlockSpec(memory_space=pltpu.VMEM)
    dep = jax.ShapeDtypeStruct((1, 4, 2, rows, levels), f32)
    cla = jax.ShapeDtypeStruct((1, 4, 2, rows, 80), f32)
    outs = pl.pallas_call(
        functools.partial(finish_kernel, rows),
        in_specs=[vm],
        out_specs=[vm] * 4,
        out_shape=[dep, dep, cla, cla],
        scratch_shapes=[pltpu.VMEM((8, 128, 128), f32)],
        name="finish",
    )(res)
    return tuple(jnp.swapaxes(o, 3, 4) for o in outs)


def solution(mesh):
    nlon, nlat, nmem = (mesh.shape[a] for a in ("lon", "lat", "mem"))

    def body(north_vel, up_vel, dens_class, thickness, basin_id):
        res = statistics(north_vel[0], up_vel[0], dens_class[0], thickness, basin_id, nlon, nlat, nmem)
        return finish(res, *thickness.shape[:2])

    big = P("mem", None, None, "lat", "lon")
    out = P("lon", None, None, None, "lat")
    return jax.shard_map(
        body, mesh=mesh, in_specs=(big, big, big, P(None, "lat", "lon"), P("lat", "lon")),
        out_specs=(out,) * 4, check_vma=False)
```
